32 devices in a mesh: lon: 16 (over z, y, core), lat: 2 (over x).
Axes of the slice: x: 2, y: 2, z: 4, core: 2. Of those that a mesh axis runs over, the one named last changes fastest.
Arguments:
- fine_members: bfloat16 [32, 64, 256], P(None, 'lon', 'lat'), may hold values from -6 to 6
- coarse_members: bfloat16 [128, 32, 256], P(None, 'lon', 'lat'), may hold values from -6 to 6
- increments: bfloat16 [32, 64, 256], P(None, 'lon', 'lat'), may hold values from -0.59765625 to 0.59765625
- level_weights: float32 [2], replicated, may hold values from 0.5 to 2
Outputs:
- applied: float32 [32, 64, 256], P(None, 'lon', 'lat')
The draws below stay inside these ranges and needn't reach their ends.
All inputs are finite; a program needn't handle non-finite values.
Results may differ from the reference program's by a relative error of at most 0.0055.
Values may be sent and summed in bfloat16 or wider, within the bound.
A program may use at most 64 MiB of HBM per device.

```python
import math
import jax
import jax.numpy as jnp
from jax import lax

CLON = 4
CLAT = 128
KF = 32
KC = 128
NV = 32
NLON = 64
NLAT = 256
N_LON = 16
N_LAT = 2


def steps_of(stream_key, shape, pieces, smallest, high):
    gain, own = 1.0, jax.random.fold_in(stream_key, 6)
    for dim, parts in pieces:
        draws = jnp.exp(jax.random.uniform(jax.random.fold_in(own, dim), (parts,), jnp.float32, smallest / len(pieces), high / len(pieces)))
        gain = gain * jnp.repeat(draws, shape[dim] // parts).reshape([-1 if axis == dim else 1 for axis in range(len(shape))])
    return gain


def bell_draw(own_key, shape, deviation, limit, split=(), kind=jnp.bfloat16):
    array = deviation * jax.random.normal(own_key, shape, jnp.float32)
    if split:
        array = array * steps_of(own_key, shape, split, -0.22, 0.18)
    return jnp.clip(array, -limit, limit).astype(kind)


def setup_inputs(seed: int = 0) -> dict:
    keys = jax.random.split(jax.random.key(seed), 5)
    return {
        "fine_members": bell_draw(keys[0], (KF, NLON, NLAT), 1.0, 6.0, ((1, 16), (2, 2))),
        "coarse_members": bell_draw(keys[1], (KC, NLON // 2, NLAT), 1.0, 6.0, ((1, 16), (2, 2))),
        "increments": bell_draw(keys[2], (NV, NLON, NLAT), 0.1, 0.59765625, ((1, 16), (2, 2))),
        "level_weights": jnp.clip(jnp.exp(jax.random.uniform(keys[3], (2,), jnp.float32, math.log(0.5), math.log(2.0))), 0.5, 2.0),
    }


def refine(coarse):
    left_cols = coarse[:, :-1, :]
    right_cols = coarse[:, 1:, :]
    middle = 0.5 * (left_cols + right_cols)
    stacked = jnp.stack((left_cols, middle), axis=2)
    return stacked.reshape(left_cols.shape[0], 2 * left_cols.shape[1], left_cols.shape[2])


def anomalies(members):
    return (members - jnp.mean(members, axis=0, keepdims=True)).astype(jnp.bfloat16)


def profile(distance, extent):
    ratio = distance.astype(jnp.float32) / extent
    return jnp.where(jnp.abs(distance) <= extent, 1.0 - 0.75 * ratio * ratio, 0.0).astype(jnp.float32)


def reference(fine_members, coarse_members, increments, level_weights):
    lon_reach = CLON - 1
    lat_reach = CLAT // 8
    ext_width = CLAT + 2 * lat_reach
    extended = jnp.concatenate((coarse_members, coarse_members[:, :1, :]), axis=1).astype(jnp.float32)
    refined = refine(extended)
    fine_anom = anomalies(fine_members.astype(jnp.float32))
    coarse_anom = anomalies(refined)
    paired_anom = anomalies(refined[:KF])
    stacked = jnp.concatenate((fine_anom, coarse_anom, paired_anom, increments), axis=0)
    padded = jnp.pad(stacked, ((0, 0), (0, 0), (lat_reach, lat_reach)))
    padded = jnp.concatenate((padded[:, -CLON:], padded, padded[:, :CLON]), axis=1)
    lon_profile = profile(jnp.arange(3 * CLON, dtype=jnp.int32)[None, :] - CLON - jnp.arange(CLON, dtype=jnp.int32)[:, None], lon_reach)
    lat_profile = profile(jnp.arange(ext_width, dtype=jnp.int32)[None, :] - lat_reach - jnp.arange(CLAT, dtype=jnp.int32)[:, None], lat_reach)
    taper = (lon_profile[:, None, :, None] * lat_profile[None, :, None, :]).reshape(CLON * CLAT, 3 * CLON * ext_width)
    weight_fine = level_weights[0] / (KF - 1)
    weight_coarse = level_weights[1] / (KC - 1)
    weight_paired = level_weights[1] / (KF - 1)
    member_rows = 2 * KF + KC
    total_rows = member_rows + NV

    def one_tile(index):
        lon_tile = index // N_LAT
        lat_tile = index % N_LAT
        zero_start = jnp.int32(0)
        hood = lax.dynamic_slice(padded, (zero_start, (lon_tile * CLON).astype(jnp.int32), (lat_tile * CLAT).astype(jnp.int32)), (total_rows, 3 * CLON, ext_width))
        own = lax.dynamic_slice(stacked, (zero_start, (lon_tile * CLON).astype(jnp.int32), (lat_tile * CLAT).astype(jnp.int32)), (member_rows, CLON, CLAT))
        hood = hood.reshape(total_rows, 3 * CLON * ext_width)
        own = own.reshape(member_rows, CLON * CLAT)
        first = jnp.dot(own[:KF].T, hood[:KF], preferred_element_type=jnp.float32)
        second = jnp.dot(own[KF:KF + KC].T, hood[KF:KF + KC], preferred_element_type=jnp.float32)
        third = jnp.dot(own[KF + KC:].T, hood[KF + KC:member_rows], preferred_element_type=jnp.float32)
        gram_tile = weight_fine * first + weight_coarse * second - weight_paired * third
        tapered = (taper * gram_tile).astype(jnp.bfloat16)
        return jnp.dot(hood[member_rows:], tapered.T, preferred_element_type=jnp.float32)

    results = lax.map(one_tile, jnp.arange(N_LON * N_LAT, dtype=jnp.int32))
    results = results.reshape(N_LON, N_LAT, NV, CLON, CLAT)
    return jnp.transpose(results, (2, 0, 3, 1, 4)).reshape(NV, N_LON * CLON, N_LAT * CLAT)
```

```python
import functools

import jax
import jax.numpy as jnp
from jax import lax
from jax.experimental import pallas as pl
from jax.experimental.pallas import tpu as pltpu
from jax.sharding import PartitionSpec as P

MESH = pl.DeviceIdType.MESH
F32, BF16 = jnp.float32, jnp.bfloat16


def profile(distance, extent):
    ratio = distance.astype(F32) / extent
    return jnp.where(jnp.abs(distance) <= extent, 1.0 - 0.75 * ratio * ratio, 0.0)


def iota(shape, dim):
    return lax.broadcasted_iota(jnp.int32, shape, dim)


def kernel(
    sizes, weights_ref, fine_ref, coarse_ref, inc_ref, out_ref,
    w_ref, fine_in, coarse_in, inc_in, wide, wide_c, west_cin, east_cin, rim_out, rim_in,
    near_f, near_c, near_p, near_i, own_t, taper, rim_taper, refine_rim, acc,
    in_sem, send_sem, recv_sem, rim_send_sem, rim_recv_sem, ok_sem,
):
    n_lon, n_lat, kf, kc, nv, lons, lats = sizes
    halves, reach, lon_reach = lons // 2, lats // 8, lons - 1
    groups = kc // kf
    ratio = (kc - 1) / (kf - 1)
    lon, lat = lax.axis_index("lon"), lax.axis_index("lat")
    sides = (lax.rem(lon + n_lon - 1, n_lon), lon, lax.rem(lon + 1, n_lon))
    has = (lat > 0, lat < n_lat - 1)
    odd = lax.rem(lat, 2) == 1
    even = jnp.logical_not(odd)
    one_side = n_lat == 2
    slots = range(1) if one_side else range(2)

    barrier = pltpu.get_barrier_semaphore()

    loads = [
        pltpu.make_async_copy(src, dst, in_sem.at[n])
        for n, (src, dst) in enumerate(
            ((coarse_ref, coarse_in), (fine_ref, fine_in), (inc_ref, inc_in), (weights_ref, w_ref))
        )
    ]
    for load in loads:
        load.start()

    def greet(to_lon, to_lat):
        pl.semaphore_signal(barrier, inc=1, device_id=(to_lon, to_lat), device_id_type=MESH)

    greet(sides[0], lat)
    greet(sides[2], lat)

    def by_side(do):
        for s in range(2):
            pl.when(has[s])(functools.partial(do, s))

    def send(src, dst, n, towards):
        return pltpu.make_async_remote_copy(
            src_ref=src, dst_ref=dst, send_sem=send_sem.at[n], recv_sem=recv_sem.at[n],
            device_id=(sides[towards], lat), device_id_type=MESH,
        )

    first, past, last = lon_reach, lon_reach + lons, 2 * lon_reach + lons
    to_west, to_east = pl.ds(first, lon_reach), pl.ds(first + 1, lon_reach)
    from_west, from_east = pl.ds(0, lon_reach), pl.ds(past, lon_reach)
    coarse_west = send(coarse_in, east_cin, 0, 0)
    coarse_east = send(coarse_in, west_cin, 1, 2)
    fine_west = send(near_f.at[to_west], near_f.at[from_east], 2, 0)
    fine_east = send(near_f.at[to_east], near_f.at[from_west], 3, 2)
    inc_west = send(near_i.at[to_west], near_i.at[from_east], 4, 0)
    inc_east = send(near_i.at[to_east], near_i.at[from_west], 5, 2)

    def rim_copy(slot, t):
        s, towards = (jnp.where(has[0], 0, 1), 1 - 2 * lat) if one_side else (slot, 2 * slot - 1)
        other = 0 if one_side else 1 - slot
        return pltpu.make_async_remote_copy(
            src_ref=rim_out.at[s], dst_ref=rim_in.at[other, 2 - t],
            send_sem=rim_send_sem.at[slot, t], recv_sem=rim_recv_sem.at[other, 2 - t],
            device_id=(sides[t], lat + towards), device_id_type=MESH,
        )

    def by_slot(do):
        for slot in slots:
            if one_side:
                do(slot)
            else:
                pl.when(has[slot])(functools.partial(do, slot))

    def rims_start(slot):
        for t in (2, 0, 1):
            rim_copy(slot, t).start()

    def rims_arrive(slot):
        for t in range(3):
            rim_copy(slot if one_side else 1 - slot, 2 - t).wait_recv()

    def rims_sent(slot):
        for t in range(3):
            rim_copy(slot, t).wait_send()

    loads[0].wait()

    @pl.when(even)
    def _():
        pl.semaphore_wait(barrier, 2)
        coarse_west.start()
        coarse_east.start()
        by_side(lambda s: greet(lon, lat + 2 * s - 1))

    def columns(source, slot):
        wide_c[slot] = source[...].astype(F32)
        return [wide_c[slot, pl.ds(c, kc, stride=halves), :] for c in range(halves)]

    f_at, i_at = 0, kf * lons
    loads[1].wait()
    wide[f_at:f_at + kf * lons] = fine_in[...].astype(F32)
    loads[2].wait()
    wide[i_at:i_at + nv * lons] = inc_in[...].astype(F32)
    fine_own, inc_own = [], []
    for a in range(lons):
        values = wide[pl.ds(f_at + a, kf, stride=lons), :]
        anom = (values - jnp.mean(values, axis=0, keepdims=True)).astype(BF16)
        vectors = wide[pl.ds(i_at + a, nv, stride=lons), :].astype(BF16)
        near_f[first + a] = anom
        near_i[first + a] = vectors
        fine_own.append(anom)
        inc_own.append(vectors)

    @pl.when(even)
    def _():
        fine_west.start()
        fine_east.start()
        inc_west.start()
        inc_east.start()

    coarse_own = columns(coarse_in, 0)
    lane = iota((kf, lats), 1)
    packs = (
        [v.astype(F32) for v in fine_own] + [v.astype(F32) for v in inc_own],
        [coarse_own[c][g * kf:(g + 1) * kf] for g in range(groups) for c in range(halves)],
    )
    for part in range(2):
        low = high = jnp.zeros((kf, lats), F32)
        for q, values in enumerate(packs[part]):
            here = (lane // reach) == q
            low = jnp.where(here, pltpu.roll(values, (reach * q) % lats, 1), low)
            high = jnp.where(here, pltpu.roll(values, (reach * (q + 1)) % lats, 1), high)
        rim_out[0, part * kf:(part + 1) * kf] = low.astype(BF16)
        rim_out[1, part * kf:(part + 1) * kf] = high.astype(BF16)

    if not one_side:
        for s in slots:
            @pl.when(jnp.logical_not(has[s]))
            def _():
                rim_in[s] = jnp.zeros(rim_in.shape[1:], BF16)

    one = jnp.int32(1)

    @pl.when(odd)
    def _():
        pl.semaphore_wait(barrier, 2 + jnp.where(has[0], one, 0) + jnp.where(has[1], one, 0))
        by_slot(rims_start)
        coarse_west.start()
        coarse_east.start()
        fine_west.start()
        fine_east.start()
        inc_west.start()
        inc_east.start()
        by_side(lambda s: pl.semaphore_signal(
            ok_sem.at[1 - s], inc=1, device_id=(lon, lat + 2 * s - 1), device_id_type=MESH
        ))

    def even_rims():
        @pl.when(even)
        def _():
            by_side(lambda s: pl.semaphore_wait(ok_sem.at[s], 1))
            by_slot(rims_start)

    loads[3].wait()
    w_coarse = w_ref[1] / (kc - 1)
    fine_ratio = ratio * w_ref[0] / w_ref[1]
    lat_profile = w_coarse * profile(iota((lats, lats), 0) - iota((lats, lats), 1), reach)
    for d in range(lon_reach + 1):
        taper[d] = lat_profile * (1.0 - 0.75 * (d / lon_reach) * (d / lon_reach))

    block = lons * reach
    shape = (2 * block, lats)
    row, lane = iota(shape, 0), iota(shape, 1)
    side, a_row, i_row = row // block, (row % block) // reach, row % reach
    b_lane, l_lane = lane // reach, lane % reach
    d_lat = reach + (2 * side - 1) * (l_lane - i_row)
    for slot in slots:
        mine = side == (jnp.where(has[0], 0, 1) if one_side else slot)
        in_lat = jnp.where(mine & (b_lane < lons), w_coarse * profile(d_lat, reach), 0.0)
        for t in range(3):
            d_lon = (t - 1) * lons + b_lane - a_row
            rim_taper[slot, :, t * lats:(t + 1) * lats] = in_lat * profile(d_lon, lon_reach)

    shape = (2 * lats, lats)
    row, lane = iota(shape, 0), iota(shape, 1)
    place = (row // lats) * halves + (row // reach) % halves
    step = jnp.abs(2 * place - lane // reach)
    weight = jnp.where(step == 0, 1.0, jnp.where(step == 1, 0.5, 0.0))
    weight = jnp.where((row % reach == lane % reach) & (lane < block), weight, 0.0)
    for g in range(groups):
        mine = (row % lats) // (reach * halves) == g
        refine_rim[:, g * lats:(g + 1) * lats] = jnp.where(mine, weight, 0.0).astype(BF16)

    def coarse_parts(refined):
        coarse_anom = refined - jnp.mean(refined, axis=0, keepdims=True)
        pair = refined[:kf]
        paired = pair - jnp.mean(pair, axis=0, keepdims=True)
        return coarse_anom.astype(BF16), paired.astype(BF16)

    def set_near(b, refined):
        coarse_anom, paired = coarse_parts(refined)
        near_c[first + b] = coarse_anom
        near_p[first + b] = paired
        return coarse_anom, paired

    def set_own(a, refined):
        coarse_anom, paired = set_near(a, refined)
        parts = [
            fine_ratio * near_f[first + a].astype(F32),
            coarse_anom.astype(F32),
            -ratio * paired.astype(F32),
        ]
        own_t[a * lats:(a + 1) * lats] = jnp.concatenate(parts, axis=0).T.astype(BF16)

    def add(b, lo, hi):
        members = jnp.concatenate([near_f[first + b], near_c[first + b], near_p[first + b]], axis=0)
        gram = jnp.dot(own_t[lo * lats:hi * lats], members, preferred_element_type=F32)
        tapered = jnp.concatenate(
            [
                (gram[(a - lo) * lats:(a - lo + 1) * lats] * taper[abs(a - b)]).astype(BF16)
                for a in range(lo, hi)
            ],
            axis=0,
        )
        acc[:, lo * lats:hi * lats] += lax.dot_general(
            near_i[first + b], tapered, (((1,), (1,)), ((), ())), preferred_element_type=F32
        )

    def middle(cols, b):
        return cols[b // 2] if b % 2 == 0 else 0.5 * (cols[b // 2] + cols[b // 2 + 1])

    acc[...] = jnp.zeros_like(acc)
    for a in range(lon_reach):
        set_own(a, middle(coarse_own, a))
    for b in range(lon_reach):
        add(b, 0, lon_reach)

    def east_coarse():
        coarse_west.wait_recv()
        east_c = columns(east_cin, 1)
        own_last = wide_c[0, pl.ds(halves - 1, kc, stride=halves), :]
        set_own(lon_reach, 0.5 * (own_last + east_c[0]))
        for b in range(lon_reach):
            set_near(lons + b, middle(east_c, b))
        add(lon_reach, 0, lons)
        for b in range(lon_reach):
            add(b, lon_reach, lons)

    def east_arrive():
        fine_west.wait_recv()
        inc_west.wait_recv()

    def east_rest():
        for b in range(lon_reach):
            add(lons + b, b + 1, lons)

    def west_coarse():
        coarse_east.wait_recv()
        west_c = columns(west_cin, 2)
        west_c.append(wide_c[0, pl.ds(0, kc, stride=halves), :])
        for b in range(1, lons):
            set_near(b - lons, middle(west_c, b))

    def west_arrive():
        fine_east.wait_recv()
        inc_east.wait_recv()

    def west_rest():
        for b in range(1, lons):
            add(b - lons, 0, b)

    def rim_members(slot):
        pairs = [
            jnp.concatenate((rim_in[slot, t, kf:], rim_in[slot, min(t + 1, 2), kf:]), axis=1)
            for t in range(3)
        ]
        refined_rim = jnp.dot(
            jnp.concatenate(pairs, axis=0), refine_rim[...], preferred_element_type=F32
        )
        members, vectors = [], []
        for t in range(3):
            refined = jnp.concatenate(
                [
                    refined_rim[t * kf:(t + 1) * kf, g * lats:(g + 1) * lats]
                    for g in range(groups)
                ],
                axis=0,
            )
            coarse_anom, paired = coarse_parts(refined)
            fine_anom = rim_in[slot, t, :kf]
            members.append(jnp.concatenate([fine_anom, coarse_anom, paired], axis=0))
            vectors.append(pltpu.roll(fine_anom.astype(F32), lats - block, 1).astype(BF16))
        return jnp.concatenate(members, axis=1), jnp.concatenate(vectors, axis=1)

    def finish(arrive, rest):
        by_slot(rims_arrive)
        rims = [rim_members(slot) for slot in slots]
        arrive()
        rest()
        own_rim = jnp.concatenate(
            [
                own_t[a * lats + s * (lats - reach):a * lats + s * (lats - reach) + reach]
                for s in range(2)
                for a in range(lons)
            ],
            axis=0,
        )
        edge = None
        for slot in slots:
            members, vectors = rims[slot]
            gram = jnp.dot(own_rim, members, preferred_element_type=F32)
            tapered = (gram * rim_taper[slot]).astype(BF16)
            part = lax.dot_general(
                vectors, tapered, (((1,), (1,)), ((), ())), preferred_element_type=F32
            )
            edge = part if edge is None else edge + part
        lane = iota((nv, lats), 1)
        for a in range(lons):
            low = pltpu.roll(edge, (lats - reach * a) % lats, 1)
            high = pltpu.roll(edge, (2 * lats - reach - block - reach * a) % lats, 1)
            total = acc[:, a * lats:(a + 1) * lats]
            total += jnp.where(lane < reach, low, 0.0) + jnp.where(lane >= lats - reach, high, 0.0)
            out_ref[pl.ds(a, nv, stride=lons), :] = total

    @pl.when(lax.rem(lon, 2) == 0)
    def _():
        east_coarse()
        east_arrive()
        east_rest()
        even_rims()
        west_coarse()
        finish(west_arrive, west_rest)

    @pl.when(lax.rem(lon, 2) == 1)
    def _():
        even_rims()
        west_coarse()
        west_arrive()
        west_rest()
        east_coarse()
        finish(east_arrive, east_rest)

    for copy in (coarse_west, coarse_east, fine_west, fine_east, inc_west, inc_east):
        copy.wait_send()
    by_slot(rims_sent)


def solution(mesh):
    n_lon, n_lat = mesh.shape["lon"], mesh.shape["lat"]

    def per_device(fine, coarse, inc, weights):
        kf, lons, lats = fine.shape
        kc, halves, _ = coarse.shape
        nv = inc.shape[0]
        members, near_lons = 2 * kf + kc, 3 * lons - 2
        slots = 1 if n_lat == 2 else 2
        assert nv == kf and 2 * lons * (lats // 8) == lats and kc * halves == 2 * lons * kf
        assert n_lon % 2 == 0
        result = pl.pallas_call(
            functools.partial(kernel, (n_lon, n_lat, kf, kc, nv, lons, lats)),
            out_shape=pltpu.VMEM((nv * lons, lats), F32),
            in_specs=[pl.BlockSpec(memory_space=pl.ANY)] * 4,
            out_specs=pl.BlockSpec(memory_space=pltpu.VMEM),
            scratch_shapes=[
                pltpu.SMEM(weights.shape, F32),
                pltpu.VMEM((kf * lons, lats), BF16),
                pltpu.VMEM((kc * halves, lats), BF16),
                pltpu.VMEM((nv * lons, lats), BF16),
                pltpu.VMEM(((kf + nv) * lons, lats), F32),
                pltpu.VMEM((3, kc * halves, lats), F32),
                pltpu.VMEM((kc * halves, lats), BF16),
                pltpu.VMEM((kc * halves, lats), BF16),
                pltpu.VMEM((2, 2 * kf, lats), BF16),
                pltpu.VMEM((slots, 3, 2 * kf, lats), BF16),
                pltpu.VMEM((near_lons, kf, lats), BF16),
                pltpu.VMEM((near_lons, kc, lats), BF16),
                pltpu.VMEM((near_lons, kf, lats), BF16),
                pltpu.VMEM((near_lons, nv, lats), BF16),
                pltpu.VMEM((lons * lats, members), BF16),
                pltpu.VMEM((lons, lats, lats), F32),
                pltpu.VMEM((slots, lats, 3 * lats), F32),
                pltpu.VMEM((2 * lats, (kc // kf) * lats), BF16),
                pltpu.VMEM((nv, lons * lats), F32),
                pltpu.SemaphoreType.DMA((4,)),
                pltpu.SemaphoreType.DMA((6,)),
                pltpu.SemaphoreType.DMA((6,)),
                pltpu.SemaphoreType.DMA((slots, 3)),
                pltpu.SemaphoreType.DMA((slots, 3)),
                pltpu.SemaphoreType.REGULAR((2,)),
            ],
            compiler_params=pltpu.CompilerParams(collective_id=0, has_side_effects=True),
            name="covariance",
        )(
            weights,
            fine.reshape(kf * lons, lats),
            coarse.reshape(kc * halves, lats),
            inc.reshape(nv * lons, lats),
        )
        return result.reshape(nv, lons, lats)

    spec = P(None, "lon", "lat")
    return jax.shard_map(
        per_device, mesh=mesh, in_specs=(spec, spec, spec, P()), out_specs=spec, check_vma=False
    )
```

```python
import functools

import jax
import jax.numpy as jnp
from jax import lax
from jax.experimental import pallas as pl
from jax.experimental.pallas import tpu as pltpu
from jax.sharding import PartitionSpec as P

MESH = pl.DeviceIdType.MESH
F32, BF16 = jnp.float32, jnp.bfloat16


def profile(distance, extent):
    ratio = distance.astype(F32) / extent
    return jnp.where(jnp.abs(distance) <= extent, 1.0 - 0.75 * ratio * ratio, 0.0)


def iota(shape, dim):
    return lax.broadcasted_iota(jnp.int32, shape, dim)


def kernel(
    sizes, weights_ref, fine_ref, coarse_ref, inc_ref, out_ref,
    w_ref, fine_in, coarse_in, inc_in, wide, wide_c, west_cin, east_cin, rim_out, rim_in,
    near_f, near_c, near_p, near_i, own_c, own_r, taper, rim_taper, refine_rim, acc,
    in_sem, send_sem, recv_sem, rim_send_sem, rim_recv_sem, ok_sem,
):
    n_lon, n_lat, kf, kc, nv, lons, lats = sizes
    halves, reach, lon_reach = lons // 2, lats // 8, lons - 1
    groups = kc // kf
    ratio = (kc - 1) / (kf - 1)
    lon, lat = lax.axis_index("lon"), lax.axis_index("lat")
    sides = (lax.rem(lon + n_lon - 1, n_lon), lon, lax.rem(lon + 1, n_lon))
    has = (lat > 0, lat < n_lat - 1)
    odd = lax.rem(lat, 2) == 1
    even = jnp.logical_not(odd)
    one_side = n_lat == 2
    slots = range(1) if one_side else range(2)

    barrier = pltpu.get_barrier_semaphore()

    loads = [
        pltpu.make_async_copy(src, dst, in_sem.at[n])
        for n, (src, dst) in enumerate(
            ((coarse_ref, coarse_in), (fine_ref, fine_in), (inc_ref, inc_in), (weights_ref, w_ref))
        )
    ]
    for load in loads:
        load.start()

    def greet(to_lon, to_lat):
        pl.semaphore_signal(barrier, inc=1, device_id=(to_lon, to_lat), device_id_type=MESH)

    greet(sides[0], lat)
    greet(sides[2], lat)

    def by_side(do):
        for s in range(2):
            if not one_side:
                pl.when(has[s])(functools.partial(do, s))
        if one_side:
            do(lax.rem(lat + 1, 2))

    def send(src, dst, n, towards):
        return pltpu.make_async_remote_copy(
            src_ref=src, dst_ref=dst, send_sem=send_sem.at[n], recv_sem=recv_sem.at[n],
            device_id=(sides[towards], lat), device_id_type=MESH,
        )

    first, past, last = lon_reach, lon_reach + lons, 2 * lon_reach + lons
    to_west, to_east = pl.ds(first, lon_reach), pl.ds(first + 1, lon_reach)
    from_west, from_east = pl.ds(0, lon_reach), pl.ds(past, lon_reach)
    coarse_west = send(coarse_in, east_cin, 0, 0)
    coarse_east = send(coarse_in, west_cin, 1, 2)
    fine_west = send(near_f.at[to_west], near_f.at[from_east], 2, 0)
    fine_east = send(near_f.at[to_east], near_f.at[from_west], 3, 2)
    inc_west = send(near_i.at[to_west], near_i.at[from_east], 4, 0)
    inc_east = send(near_i.at[to_east], near_i.at[from_west], 5, 2)

    def rim_copy(slot, t):
        s, towards = (jnp.where(has[0], 0, 1), 1 - 2 * lat) if one_side else (slot, 2 * slot - 1)
        other = 0 if one_side else 1 - slot
        return pltpu.make_async_remote_copy(
            src_ref=rim_out.at[s], dst_ref=rim_in.at[other, 2 - t],
            send_sem=rim_send_sem.at[slot, t], recv_sem=rim_recv_sem.at[other, 2 - t],
            device_id=(sides[t], lat + towards), device_id_type=MESH,
        )

    def by_slot(do):
        for slot in slots:
            if one_side:
                do(slot)
            else:
                pl.when(has[slot])(functools.partial(do, slot))

    def rims_start(slot):
        for t in (2, 0, 1):
            rim_copy(slot, t).start()

    def rims_arrive(slot):
        for t in range(3):
            rim_copy(slot if one_side else 1 - slot, 2 - t).wait_recv()

    def rims_sent(slot):
        for t in range(3):
            rim_copy(slot, t).wait_send()

    loads[0].wait()

    @pl.when(even)
    def _():
        pl.semaphore_wait(barrier, 2)
        coarse_west.start()
        coarse_east.start()
        by_side(lambda s: greet(lon, lat + 2 * s - 1))

    def columns(source, slot):
        wide_c[slot] = source[...].astype(F32)
        return [wide_c[slot, pl.ds(c, kc, stride=halves), :] for c in range(halves)]

    f_at, i_at = 0, kf * lons
    loads[1].wait()
    wide[f_at:f_at + kf * lons] = fine_in[...].astype(F32)
    loads[2].wait()
    wide[i_at:i_at + nv * lons] = inc_in[...].astype(F32)
    fine_own, inc_own = [], []
    for a in range(lons):
        values = wide[pl.ds(f_at + a, kf, stride=lons), :]
        anom = (values - jnp.mean(values, axis=0, keepdims=True)).astype(BF16)
        vectors = wide[pl.ds(i_at + a, nv, stride=lons), :].astype(BF16)
        near_f[first + a] = anom
        near_i[first + a] = vectors
        fine_own.append(anom)
        inc_own.append(vectors)

    @pl.when(even)
    def _():
        fine_west.start()
        fine_east.start()
        inc_west.start()
        inc_east.start()

    coarse_own = columns(coarse_in, 0)
    lane = iota((kf, lats), 1)
    packs = (
        [v.astype(F32) for v in fine_own] + [v.astype(F32) for v in inc_own],
        [coarse_own[c][g * kf:(g + 1) * kf] for g in range(groups) for c in range(halves)],
    )
    for part in range(2):
        low = high = jnp.zeros((kf, lats), F32)
        for q, values in enumerate(packs[part]):
            here = (lane // reach) == q
            low = jnp.where(here, pltpu.roll(values, (reach * q) % lats, 1), low)
            high = jnp.where(here, pltpu.roll(values, (reach * (q + 1)) % lats, 1), high)
        rim_out[0, part * kf:(part + 1) * kf] = low.astype(BF16)
        rim_out[1, part * kf:(part + 1) * kf] = high.astype(BF16)

    if not one_side:
        for s in slots:
            @pl.when(jnp.logical_not(has[s]))
            def _():
                rim_in[s] = jnp.zeros(rim_in.shape[1:], BF16)

    one = jnp.int32(1)

    @pl.when(odd)
    def _():
        pl.semaphore_wait(barrier, 2 + jnp.where(has[0], one, 0) + jnp.where(has[1], one, 0))
        by_slot(rims_start)
        coarse_west.start()
        coarse_east.start()
        fine_west.start()
        fine_east.start()
        inc_west.start()
        inc_east.start()
        by_side(lambda s: pl.semaphore_signal(
            ok_sem.at[1 - s], inc=1, device_id=(lon, lat + 2 * s - 1), device_id_type=MESH
        ))

    loads[3].wait()
    w_coarse = w_ref[1] / (kc - 1)
    fine_ratio = ratio * w_ref[0] / w_ref[1]
    lat_profile = w_coarse * profile(iota((lats, lats), 0) - iota((lats, lats), 1), reach)
    for d in range(lon_reach + 1):
        taper[d] = lat_profile * (1.0 - 0.75 * (d / lon_reach) * (d / lon_reach))

    block = lons * reach
    shape = (2 * block, lats)
    row, lane = iota(shape, 0), iota(shape, 1)
    side, a_row, i_row = row // block, (row % block) // reach, row % reach
    b_lane, l_lane = lane // reach, lane % reach
    d_lat = reach + (2 * side - 1) * (l_lane - i_row)
    for slot in slots:
        mine = side == (jnp.where(has[0], 0, 1) if one_side else slot)
        in_lat = jnp.where(mine & (b_lane < lons), w_coarse * profile(d_lat, reach), 0.0)
        for t in range(3):
            d_lon = (t - 1) * lons + b_lane - a_row
            rim_taper[slot, :, t * lats:(t + 1) * lats] = in_lat * profile(d_lon, lon_reach)

    shape = (2 * lats, lats)
    row, lane = iota(shape, 0), iota(shape, 1)
    place = (row // lats) * halves + (row // reach) % halves
    step = jnp.abs(2 * place - lane // reach)
    weight = jnp.where(step == 0, 1.0, jnp.where(step == 1, 0.5, 0.0))
    weight = jnp.where((row % reach == lane % reach) & (lane < block), weight, 0.0)
    for g in range(groups):
        mine = (row % lats) // (reach * halves) == g
        refine_rim[:, g * lats:(g + 1) * lats] = jnp.where(mine, weight, 0.0).astype(BF16)

    def coarse_parts(refined):
        coarse_anom = refined - jnp.mean(refined, axis=0, keepdims=True)
        pair = refined[:kf]
        paired = pair - jnp.mean(pair, axis=0, keepdims=True)
        return coarse_anom.astype(BF16), paired.astype(BF16)

    def set_near(b, refined):
        coarse_anom, paired = coarse_parts(refined)
        near_c[first + b] = coarse_anom
        near_p[first + b] = paired
        return coarse_anom, paired

    def split(scale, values):
        scaled = scale * values.astype(F32)
        high = scaled.astype(BF16).astype(F32)
        return [high, scaled - high]

    def set_own(a, refined):
        coarse_anom, paired = set_near(a, refined)
        rest = split(fine_ratio, near_f[first + a]) + split(-ratio, paired)
        own_c[a] = coarse_anom.astype(F32).T.astype(BF16)
        own_r[a] = jnp.concatenate(rest, axis=0).T.astype(BF16)

    def own_rows(lo, hi):
        return jnp.concatenate(
            [jnp.concatenate([own_c[a], own_r[a]], axis=1) for a in range(lo, hi)], axis=0
        )

    def members(coarse_anom, fine_anom, paired):
        return jnp.concatenate([coarse_anom, fine_anom, fine_anom, paired, paired], axis=0)

    def tapered_rows(b, lo, hi):
        at = first + b
        gram = jnp.dot(
            own_rows(lo, hi), members(near_c[at], near_f[at], near_p[at]), preferred_element_type=F32
        )
        return {
            a: (gram[(a - lo) * lats:(a - lo + 1) * lats] * taper[abs(a - b)]).astype(BF16)
            for a in range(lo, hi)
        }

    def apply(rows, a):
        near = [b for b in rows if a in rows[b]]
        vectors = jnp.concatenate([near_i[first + b] for b in near], axis=1)
        tapered = jnp.concatenate([rows[b][a] for b in near], axis=1)
        return lax.dot_general(
            vectors, tapered, (((1,), (1,)), ((), ())), preferred_element_type=F32
        )

    def middle(cols, b):
        return cols[b // 2] if b % 2 == 0 else 0.5 * (cols[b // 2] + cols[b // 2 + 1])

    for a in range(lon_reach):
        set_own(a, middle(coarse_own, a))
    rows = {b: tapered_rows(b, 0, lon_reach) for b in range(lon_reach)}
    for a in range(lon_reach):
        acc[a] = apply(rows, a)

    @pl.when(even)
    def _():
        by_side(lambda s: pl.semaphore_wait(ok_sem.at[s], 1))
        by_slot(rims_start)

    coarse_west.wait_recv()
    east_c = columns(east_cin, 1)
    set_own(lon_reach, 0.5 * (coarse_own[halves - 1] + east_c[0]))
    rows = {b: tapered_rows(b, lon_reach, lons) for b in range(lon_reach)}
    rows[lon_reach] = tapered_rows(lon_reach, 0, lons)
    for b in range(lon_reach):
        set_near(lons + b, middle(east_c, b))
    for a in range(lon_reach):
        acc[a] += apply(rows, a)
    acc[lon_reach] = apply(rows, lon_reach)
    fine_west.wait_recv()
    inc_west.wait_recv()
    rows = {lons + b: tapered_rows(lons + b, b + 1, lons) for b in range(lon_reach)}
    for a in range(1, lons):
        acc[a] += apply(rows, a)

    coarse_east.wait_recv()
    west_c = columns(west_cin, 2)
    west_c.append(coarse_own[0])
    for b in range(1, lons):
        set_near(b - lons, middle(west_c, b))

    def rim_members(slot):
        pairs = [
            jnp.concatenate((rim_in[slot, t, kf:], rim_in[slot, min(t + 1, 2), kf:]), axis=1)
            for t in range(3)
        ]
        refined_rim = jnp.dot(
            jnp.concatenate(pairs, axis=0), refine_rim[...], preferred_element_type=F32
        )
        cells, vectors = [], []
        for t in range(3):
            refined = jnp.concatenate(
                [
                    refined_rim[t * kf:(t + 1) * kf, g * lats:(g + 1) * lats]
                    for g in range(groups)
                ],
                axis=0,
            )
            coarse_anom, paired = coarse_parts(refined)
            fine_anom = rim_in[slot, t, :kf]
            cells.append(members(coarse_anom, fine_anom, paired))
            vectors.append(pltpu.roll(fine_anom.astype(F32), lats - block, 1).astype(BF16))
        return jnp.concatenate(cells, axis=1), jnp.concatenate(vectors, axis=1)

    by_slot(rims_arrive)
    rims = [rim_members(slot) for slot in slots]
    fine_east.wait_recv()
    inc_east.wait_recv()
    rows = {b - lons: tapered_rows(b - lons, 0, b) for b in range(1, lons)}
    total = [acc[a] + apply(rows, a) for a in range(lon_reach)] + [acc[lon_reach]]
    own_rim = jnp.concatenate(
        [
            jnp.concatenate(
                [own[a, s * (lats - reach):s * (lats - reach) + reach] for own in (own_c, own_r)],
                axis=1,
            )
            for s in range(2)
            for a in range(lons)
        ],
        axis=0,
    )
    edge = None
    for slot in slots:
        cells, vectors = rims[slot]
        gram = jnp.dot(own_rim, cells, preferred_element_type=F32)
        tapered = (gram * rim_taper[slot]).astype(BF16)
        part = lax.dot_general(
            vectors, tapered, (((1,), (1,)), ((), ())), preferred_element_type=F32
        )
        edge = part if edge is None else edge + part
    lane = iota((nv, lats), 1)
    for a in range(lons):
        low = pltpu.roll(edge, (lats - reach * a) % lats, 1)
        high = pltpu.roll(edge, (2 * lats - reach - block - reach * a) % lats, 1)
        rim = jnp.where(lane < reach, low, 0.0) + jnp.where(lane >= lats - reach, high, 0.0)
        out_ref[pl.ds(a, nv, stride=lons), :] = total[a] + rim

    for copy in (coarse_west, coarse_east, fine_west, fine_east, inc_west, inc_east):
        copy.wait_send()
    by_slot(rims_sent)


def solution(mesh):
    n_lon, n_lat = mesh.shape["lon"], mesh.shape["lat"]

    def per_device(fine, coarse, inc, weights):
        kf, lons, lats = fine.shape
        kc, halves, _ = coarse.shape
        nv = inc.shape[0]
        near_lons = 3 * lons - 2
        slots = 1 if n_lat == 2 else 2
        assert nv == kf and 2 * lons * (lats // 8) == lats and kc * halves == 2 * lons * kf
        result = pl.pallas_call(
            functools.partial(kernel, (n_lon, n_lat, kf, kc, nv, lons, lats)),
            out_shape=pltpu.VMEM((nv * lons, lats), F32),
            in_specs=[pl.BlockSpec(memory_space=pl.ANY)] * 4,
            out_specs=pl.BlockSpec(memory_space=pltpu.VMEM),
            scratch_shapes=[
                pltpu.SMEM(weights.shape, F32),
                pltpu.VMEM((kf * lons, lats), BF16),
                pltpu.VMEM((kc * halves, lats), BF16),
                pltpu.VMEM((nv * lons, lats), BF16),
                pltpu.VMEM(((kf + nv) * lons, lats), F32),
                pltpu.VMEM((3, kc * halves, lats), F32),
                pltpu.VMEM((kc * halves, lats), BF16),
                pltpu.VMEM((kc * halves, lats), BF16),
                pltpu.VMEM((2, 2 * kf, lats), BF16),
                pltpu.VMEM((slots, 3, 2 * kf, lats), BF16),
                pltpu.VMEM((near_lons, kf, lats), BF16),
                pltpu.VMEM((near_lons, kc, lats), BF16),
                pltpu.VMEM((near_lons, kf, lats), BF16),
                pltpu.VMEM((near_lons, nv, lats), BF16),
                pltpu.VMEM((lons, lats, kc), BF16),
                pltpu.VMEM((lons, lats, 4 * kf), BF16),
                pltpu.VMEM((lons, lats, lats), F32),
                pltpu.VMEM((slots, lats, 3 * lats), F32),
                pltpu.VMEM((2 * lats, (kc // kf) * lats), BF16),
                pltpu.VMEM((lons, nv, lats), F32),
                pltpu.SemaphoreType.DMA((4,)),
                pltpu.SemaphoreType.DMA((6,)),
                pltpu.SemaphoreType.DMA((6,)),
                pltpu.SemaphoreType.DMA((slots, 3)),
                pltpu.SemaphoreType.DMA((slots, 3)),
                pltpu.SemaphoreType.REGULAR((2,)),
            ],
            compiler_params=pltpu.CompilerParams(collective_id=0, has_side_effects=True),
            name="covariance",
        )(
            weights,
            fine.reshape(kf * lons, lats),
            coarse.reshape(kc * halves, lats),
            inc.reshape(nv * lons, lats),
        )
        return result.reshape(nv, lons, lats)

    spec = P(None, "lon", "lat")
    return jax.shard_map(
        per_device, mesh=mesh, in_specs=(spec, spec, spec, P()), out_specs=spec, check_vma=False
    )
```

```python
import functools

import jax
import jax.numpy as jnp
from jax import lax
from jax.experimental import pallas as pl
from jax.experimental.pallas import tpu as pltpu
from jax.sharding import PartitionSpec as P

MESH = pl.DeviceIdType.MESH
F32, BF16 = jnp.float32, jnp.bfloat16


def profile(distance, extent):
    ratio = distance.astype(F32) / extent
    return jnp.where(jnp.abs(distance) <= extent, 1.0 - 0.75 * ratio * ratio, 0.0)


def iota(shape, dim):
    return lax.broadcasted_iota(jnp.int32, shape, dim)


def kernel(
    sizes, weights_ref, fine_ref, coarse_ref, inc_ref, out_ref,
    w_ref, fine_in, coarse_in, inc_in, wide, wide_c, west_cin, east_cin, rim_out, rim_in,
    near_v, near_c, near_p, own_c, own_r, taper, rim_taper, refine_rim, acc,
    in_sem, send_sem, recv_sem, rim_send_sem, rim_recv_sem, ok_sem,
):
    n_lon, n_lat, kf, kc, nv, lons, lats = sizes
    halves, reach, lon_reach = lons // 2, lats // 8, lons - 1
    groups = kc // kf
    ratio = (kc - 1) / (kf - 1)
    lon, lat = lax.axis_index("lon"), lax.axis_index("lat")
    sides = (lax.rem(lon + n_lon - 1, n_lon), lon, lax.rem(lon + 1, n_lon))
    has = (lat > 0, lat < n_lat - 1)
    odd = lax.rem(lat, 2) == 1
    even = jnp.logical_not(odd)
    one_side = n_lat == 2
    slots = range(1) if one_side else range(2)

    barrier = pltpu.get_barrier_semaphore()

    loads = [
        pltpu.make_async_copy(src, dst, in_sem.at[n])
        for n, (src, dst) in enumerate(
            ((coarse_ref, coarse_in), (fine_ref, fine_in), (inc_ref, inc_in), (weights_ref, w_ref))
        )
    ]
    for load in loads:
        load.start()

    def by_side(do):
        for s in range(2):
            if not one_side:
                pl.when(has[s])(functools.partial(do, s))
        if one_side:
            do(lax.rem(lat + 1, 2))

    def greet(to_lon, to_lat):
        pl.semaphore_signal(barrier, inc=1, device_id=(to_lon, to_lat), device_id_type=MESH)

    greet(sides[0], lat)
    greet(sides[2], lat)

    @pl.when(even)
    def _():
        by_side(lambda s: [greet(sides[t], lat + 2 * s - 1) for t in (1, 0, 2)] and None)

    def send(src, dst, n, towards):
        return pltpu.make_async_remote_copy(
            src_ref=src, dst_ref=dst, send_sem=send_sem.at[n], recv_sem=recv_sem.at[n],
            device_id=(sides[towards], lat), device_id_type=MESH,
        )

    first, past, last = lon_reach, lon_reach + lons, 2 * lon_reach + lons
    to_west, to_east = pl.ds(first, lon_reach), pl.ds(first + 1, lon_reach)
    from_west, from_east = pl.ds(0, lon_reach), pl.ds(past, lon_reach)
    coarse_west = send(coarse_in, east_cin, 0, 0)
    coarse_east = send(coarse_in, west_cin, 1, 2)
    rest_west = send(near_v.at[to_west], near_v.at[from_east], 2, 0)
    rest_east = send(near_v.at[to_east], near_v.at[from_west], 3, 2)

    def rim_copy(slot, t):
        s, towards = (jnp.where(has[0], 0, 1), 1 - 2 * lat) if one_side else (slot, 2 * slot - 1)
        other = 0 if one_side else 1 - slot
        return pltpu.make_async_remote_copy(
            src_ref=rim_out.at[s], dst_ref=rim_in.at[other, 2 - t],
            send_sem=rim_send_sem.at[slot, t], recv_sem=rim_recv_sem.at[other, 2 - t],
            device_id=(lax.rem(lon + n_lon - 1 + t, n_lon), lat + towards), device_id_type=MESH,
        )

    def by_slot(do):
        for slot in slots:
            if one_side:
                do(slot)
            else:
                pl.when(has[slot])(functools.partial(do, slot))

    def rims_start(slot):
        ahead = lax.rem(lon, 2)
        for t in (1 + ahead, 2 - ahead, 0):
            rim_copy(slot, t).start()

    def rims_arrive(slot):
        for t in range(3):
            rim_copy(slot if one_side else 1 - slot, 2 - t).wait_recv()

    def rims_sent(slot):
        for t in range(3):
            rim_copy(slot, t).wait_send()

    loads[0].wait()

    @pl.when(even)
    def _():
        pl.semaphore_wait(barrier, 2)
        coarse_west.start()
        coarse_east.start()

    def columns(source, slot):
        wide_c[slot] = source[...].astype(F32)
        return [wide_c[slot, pl.ds(c, kc, stride=halves), :] for c in range(halves)]

    f_at, i_at = 0, kf * lons
    loads[1].wait()
    wide[f_at:f_at + kf * lons] = fine_in[...].astype(F32)
    loads[2].wait()
    wide[i_at:i_at + nv * lons] = inc_in[...].astype(F32)
    fine_own, inc_own = [], []
    for a in range(lons):
        values = wide[pl.ds(f_at + a, kf, stride=lons), :]
        anom = (values - jnp.mean(values, axis=0, keepdims=True)).astype(BF16)
        vectors = wide[pl.ds(i_at + a, nv, stride=lons), :].astype(BF16)
        near_v[first + a, :kf] = anom
        near_v[first + a, kf:] = vectors
        fine_own.append(anom)
        inc_own.append(vectors)

    @pl.when(even)
    def _():
        rest_west.start()
        rest_east.start()

    coarse_own = columns(coarse_in, 0)
    lane = iota((kf, lats), 1)
    packs = (
        [v.astype(F32) for v in fine_own] + [v.astype(F32) for v in inc_own],
        [coarse_own[c][g * kf:(g + 1) * kf] for g in range(groups) for c in range(halves)],
    )
    for part in range(2):
        low = high = jnp.zeros((kf, lats), F32)
        for q, values in enumerate(packs[part]):
            here = (lane // reach) == q
            low = jnp.where(here, pltpu.roll(values, (reach * q) % lats, 1), low)
            high = jnp.where(here, pltpu.roll(values, (reach * (q + 1)) % lats, 1), high)
        rim_out[0, part * kf:(part + 1) * kf] = low.astype(BF16)
        rim_out[1, part * kf:(part + 1) * kf] = high.astype(BF16)

    if not one_side:
        for s in slots:
            @pl.when(jnp.logical_not(has[s]))
            def _():
                rim_in[s] = jnp.zeros(rim_in.shape[1:], BF16)

    one = jnp.int32(1)

    @pl.when(odd)
    def _():
        pl.semaphore_wait(barrier, 2 + 3 * jnp.where(has[0], one, 0) + 3 * jnp.where(has[1], one, 0))
        by_slot(rims_start)
        coarse_west.start()
        coarse_east.start()
        rest_west.start()
        rest_east.start()
        by_side(lambda s: pl.semaphore_signal(
            ok_sem.at[0 if one_side else 1 - s], inc=1, device_id=(lon, lat + 2 * s - 1), device_id_type=MESH
        ))

    loads[3].wait()
    w_coarse = w_ref[1] / (kc - 1)
    fine_ratio = ratio * w_ref[0] / w_ref[1]
    lat_profile = w_coarse * profile(iota((lats, lats), 0) - iota((lats, lats), 1), reach)
    for d in range(lon_reach + 1):
        taper[d] = lat_profile * (1.0 - 0.75 * (d / lon_reach) * (d / lon_reach))

    block = lons * reach
    shape = (2 * block, lats)
    row, lane = iota(shape, 0), iota(shape, 1)
    side, a_row, i_row = row // block, (row % block) // reach, row % reach
    b_lane, l_lane = lane // reach, lane % reach
    d_lat = reach + (2 * side - 1) * (l_lane - i_row)
    for slot in slots:
        mine = side == (jnp.where(has[0], 0, 1) if one_side else slot)
        in_lat = jnp.where(mine & (b_lane < lons), w_coarse * profile(d_lat, reach), 0.0)
        for t in range(3):
            d_lon = (t - 1) * lons + b_lane - a_row
            rim_taper[slot, :, t * lats:(t + 1) * lats] = in_lat * profile(d_lon, lon_reach)

    shape = (2 * lats, lats)
    row, lane = iota(shape, 0), iota(shape, 1)
    place = (row // lats) * halves + (row // reach) % halves
    step = jnp.abs(2 * place - lane // reach)
    weight = jnp.where(step == 0, 1.0, jnp.where(step == 1, 0.5, 0.0))
    weight = jnp.where((row % reach == lane % reach) & (lane < block), weight, 0.0)
    for g in range(groups):
        mine = (row % lats) // (reach * halves) == g
        refine_rim[:, g * lats:(g + 1) * lats] = jnp.where(mine, weight, 0.0).astype(BF16)

    def coarse_parts(refined):
        coarse_anom = refined - jnp.mean(refined, axis=0, keepdims=True)
        pair = refined[:kf]
        paired = pair - jnp.mean(pair, axis=0, keepdims=True)
        return coarse_anom.astype(BF16), paired.astype(BF16)

    def set_near(b, refined):
        coarse_anom, paired = coarse_parts(refined)
        near_c[first + b] = coarse_anom
        near_p[first + b] = paired
        return coarse_anom, paired

    def split(scale, values):
        scaled = scale * values.astype(F32)
        high = scaled.astype(BF16).astype(F32)
        return [high, scaled - high]

    def set_own(a, refined):
        coarse_anom, paired = set_near(a, refined)
        rest = split(fine_ratio, near_v[first + a, :kf]) + split(-ratio, paired)
        own_c[a] = coarse_anom.astype(F32).T.astype(BF16)
        own_r[a] = jnp.concatenate(rest, axis=0).T.astype(BF16)

    def own_rows(lo, hi):
        return jnp.concatenate(
            [jnp.concatenate([own_c[a], own_r[a]], axis=1) for a in range(lo, hi)], axis=0
        )

    def members(coarse_anom, fine_anom, paired):
        return jnp.concatenate([coarse_anom, fine_anom, fine_anom, paired, paired], axis=0)

    def near(b):
        at = first + b
        return members(near_c[at], near_v[at, :kf], near_p[at])

    def product(rows, bs, lo, hi):
        gram = jnp.dot(
            own_rows(lo, hi), jnp.concatenate([near(b) for b in bs], axis=1),
            preferred_element_type=F32,
        )
        for n, b in enumerate(bs):
            for a in range(lo, hi):
                part = gram[(a - lo) * lats:(a - lo + 1) * lats, n * lats:(n + 1) * lats]
                rows[a, b] = (part * taper[abs(a - b)]).astype(BF16)

    def apply(rows, a):
        bs = sorted(b for row, b in rows if row == a)
        vectors = jnp.concatenate([near_v[first + b, kf:] for b in bs], axis=1)
        tapered = jnp.concatenate([rows[a, b] for b in bs], axis=1)
        return lax.dot_general(
            vectors, tapered, (((1,), (1,)), ((), ())), preferred_element_type=F32
        )

    def middle(cols, b):
        return cols[b // 2] if b % 2 == 0 else 0.5 * (cols[b // 2] + cols[b // 2 + 1])

    for a in range(lon_reach):
        set_own(a, middle(coarse_own, a))
    rows = {}
    product(rows, tuple(range(lon_reach)), 0, lon_reach)
    for a in range(lon_reach):
        acc[a] = apply(rows, a)

    @pl.when(even)
    def _():
        by_side(lambda s: pl.semaphore_wait(ok_sem.at[0 if one_side else s], 1))
        by_slot(rims_start)

    coarse_west.wait_recv()
    east_c = columns(east_cin, 1)
    set_own(lon_reach, 0.5 * (coarse_own[halves - 1] + east_c[0]))
    rows = {}
    product(rows, tuple(range(lon_reach)), lon_reach, lons)
    product(rows, (lon_reach,), 0, lons)
    for b in range(lon_reach):
        set_near(lons + b, middle(east_c, b))
    for a in range(lon_reach):
        acc[a] += apply(rows, a)
    acc[lon_reach] = apply(rows, lon_reach)
    rest_west.wait_recv()
    rows = {}
    for b in range(0, lon_reach, 2):
        pair = tuple(lons + n for n in range(b, min(b + 2, lon_reach)))
        if len(pair) == 2:
            product(rows, pair[:1], b + 1, b + 2)
        product(rows, pair, b + len(pair), lons)
    for a in range(1, lons):
        acc[a] += apply(rows, a)

    coarse_east.wait_recv()
    west_c = columns(west_cin, 2)
    west_c.append(coarse_own[0])
    for b in range(1, lons):
        set_near(b - lons, middle(west_c, b))

    def rim_members(slot):
        pairs = [
            jnp.concatenate((rim_in[slot, t, kf:], rim_in[slot, min(t + 1, 2), kf:]), axis=1)
            for t in range(3)
        ]
        refined_rim = jnp.dot(
            jnp.concatenate(pairs, axis=0), refine_rim[...], preferred_element_type=F32
        )
        cells, vectors = [], []
        for t in range(3):
            refined = jnp.concatenate(
                [
                    refined_rim[t * kf:(t + 1) * kf, g * lats:(g + 1) * lats]
                    for g in range(groups)
                ],
                axis=0,
            )
            coarse_anom, paired = coarse_parts(refined)
            fine_anom = rim_in[slot, t, :kf]
            cells.append(members(coarse_anom, fine_anom, paired))
            vectors.append(pltpu.roll(fine_anom.astype(F32), lats - block, 1).astype(BF16))
        return jnp.concatenate(cells, axis=1), jnp.concatenate(vectors, axis=1)

    rest_east.wait_recv()
    by_slot(rims_arrive)
    rims = [rim_members(slot) for slot in slots]
    rows = {}
    for b in range(lons - 1, 0, -2):
        pair = tuple(n - lons for n in range(b, max(b - 2, 0), -1))
        product(rows, pair, 0, b + 1 - len(pair))
        if len(pair) == 2:
            product(rows, pair[:1], b - 1, b)
    total = [acc[a] + apply(rows, a) for a in range(lon_reach)] + [acc[lon_reach]]
    own_rim = jnp.concatenate(
        [
            jnp.concatenate(
                [own[a, s * (lats - reach):s * (lats - reach) + reach] for own in (own_c, own_r)],
                axis=1,
            )
            for s in range(2)
            for a in range(lons)
        ],
        axis=0,
    )
    edge = None
    for slot in slots:
        cells, vectors = rims[slot]
        gram = jnp.dot(own_rim, cells, preferred_element_type=F32)
        tapered = (gram * rim_taper[slot]).astype(BF16)
        part = lax.dot_general(
            vectors, tapered, (((1,), (1,)), ((), ())), preferred_element_type=F32
        )
        edge = part if edge is None else edge + part
    lane = iota((nv, lats), 1)
    for a in range(lons):
        low = pltpu.roll(edge, (lats - reach * a) % lats, 1)
        high = pltpu.roll(edge, (2 * lats - reach - block - reach * a) % lats, 1)
        rim = jnp.where(lane < reach, low, 0.0) + jnp.where(lane >= lats - reach, high, 0.0)
        out_ref[pl.ds(a, nv, stride=lons), :] = total[a] + rim

    for copy in (coarse_west, coarse_east, rest_west, rest_east):
        copy.wait_send()
    by_slot(rims_sent)


def solution(mesh):
    n_lon, n_lat = mesh.shape["lon"], mesh.shape["lat"]

    def per_device(fine, coarse, inc, weights):
        kf, lons, lats = fine.shape
        kc, halves, _ = coarse.shape
        nv = inc.shape[0]
        near_lons = 3 * lons - 2
        slots = 1 if n_lat == 2 else 2
        assert nv == kf and 2 * lons * (lats // 8) == lats and kc * halves == 2 * lons * kf
        result = pl.pallas_call(
            functools.partial(kernel, (n_lon, n_lat, kf, kc, nv, lons, lats)),
            out_shape=pltpu.VMEM((nv * lons, lats), F32),
            in_specs=[pl.BlockSpec(memory_space=pl.ANY)] * 4,
            out_specs=pl.BlockSpec(memory_space=pltpu.VMEM),
            scratch_shapes=[
                pltpu.SMEM(weights.shape, F32),
                pltpu.VMEM((kf * lons, lats), BF16),
                pltpu.VMEM((kc * halves, lats), BF16),
                pltpu.VMEM((nv * lons, lats), BF16),
                pltpu.VMEM(((kf + nv) * lons, lats), F32),
                pltpu.VMEM((3, kc * halves, lats), F32),
                pltpu.VMEM((kc * halves, lats), BF16),
                pltpu.VMEM((kc * halves, lats), BF16),
                pltpu.VMEM((2, 2 * kf, lats), BF16),
                pltpu.VMEM((slots, 3, 2 * kf, lats), BF16),
                pltpu.VMEM((near_lons, kf + nv, lats), BF16),
                pltpu.VMEM((near_lons, kc, lats), BF16),
                pltpu.VMEM((near_lons, kf, lats), BF16),
                pltpu.VMEM((lons, lats, kc), BF16),
                pltpu.VMEM((lons, lats, 4 * kf), BF16),
                pltpu.VMEM((lons, lats, lats), F32),
                pltpu.VMEM((slots, lats, 3 * lats), F32),
                pltpu.VMEM((2 * lats, (kc // kf) * lats), BF16),
                pltpu.VMEM((lons, nv, lats), F32),
                pltpu.SemaphoreType.DMA((4,)),
                pltpu.SemaphoreType.DMA((4,)),
                pltpu.SemaphoreType.DMA((4,)),
                pltpu.SemaphoreType.DMA((slots, 3)),
                pltpu.SemaphoreType.DMA((slots, 3)),
                pltpu.SemaphoreType.REGULAR((slots,)),
            ],
            compiler_params=pltpu.CompilerParams(collective_id=0, has_side_effects=True),
            name="covariance",
        )(
            weights,
            fine.reshape(kf * lons, lats),
            coarse.reshape(kc * halves, lats),
            inc.reshape(nv * lons, lats),
        )
        return result.reshape(nv, lons, lats)

    spec = P(None, "lon", "lat")
    return jax.shard_map(
        per_device, mesh=mesh, in_specs=(spec, spec, spec, P()), out_specs=spec, check_vma=False
    )
```

```python
import functools

import jax
import jax.numpy as jnp
from jax import lax
from jax.experimental import pallas as pl
from jax.experimental.pallas import tpu as pltpu
from jax.sharding import PartitionSpec as P

MESH = pl.DeviceIdType.MESH
F32, BF16 = jnp.float32, jnp.bfloat16


def profile(distance, extent):
    ratio = distance.astype(F32) / extent
    return jnp.where(jnp.abs(distance) <= extent, 1.0 - 0.75 * ratio * ratio, 0.0)


def iota(shape, dim):
    return lax.broadcasted_iota(jnp.int32, shape, dim)


def kernel(
    sizes, weights_ref, fine_ref, coarse_ref, inc_ref, out_ref,
    w_ref, fine_in, coarse_in, inc_in, wide, wide_c, west_cin, east_cin, rim_out, rim_in,
    near_v, near_c, near_p, own_c, own_r, taper, rim_taper, own_rim, acc,
    in_sem, send_sem, recv_sem, rim_send_sem, rim_recv_sem, ok_sem,
):
    n_lon, n_lat, kf, kc, nv, lons, lats = sizes
    halves, reach, lon_reach = lons // 2, lats // 8, lons - 1
    ratio = (kc - 1) / (kf - 1)
    lon, lat = lax.axis_index("lon"), lax.axis_index("lat")
    sides = (lax.rem(lon + n_lon - 1, n_lon), lon, lax.rem(lon + 1, n_lon))
    has = (lat > 0, lat < n_lat - 1)
    odd = lax.rem(lat, 2) == 1
    even = jnp.logical_not(odd)
    one_side = n_lat == 2
    slots = range(1) if one_side else range(2)

    barrier = pltpu.get_barrier_semaphore()

    loads = [
        pltpu.make_async_copy(src, dst, in_sem.at[n])
        for n, (src, dst) in enumerate(
            ((coarse_ref, coarse_in), (fine_ref, fine_in), (inc_ref, inc_in), (weights_ref, w_ref))
        )
    ]
    for load in loads:
        load.start()

    def by_side(do):
        for s in range(2):
            if not one_side:
                pl.when(has[s])(functools.partial(do, s))
        if one_side:
            do(lax.rem(lat + 1, 2))

    def greet(to_lon, to_lat):
        pl.semaphore_signal(barrier, inc=1, device_id=(to_lon, to_lat), device_id_type=MESH)

    greet(sides[0], lat)
    greet(sides[2], lat)

    @pl.when(even)
    def _():
        by_side(lambda s: [greet(sides[t], lat + 2 * s - 1) for t in (1, 0, 2)] and None)

    def send(src, dst, n, towards):
        return pltpu.make_async_remote_copy(
            src_ref=src, dst_ref=dst, send_sem=send_sem.at[n], recv_sem=recv_sem.at[n],
            device_id=(sides[towards], lat), device_id_type=MESH,
        )

    first, past, last = lon_reach, lon_reach + lons, 2 * lon_reach + lons
    to_west, to_east = pl.ds(first, lon_reach), pl.ds(first + 1, lon_reach)
    from_west, from_east = pl.ds(0, lon_reach), pl.ds(past, lon_reach)
    coarse_west = send(coarse_in, east_cin, 0, 0)
    coarse_east = send(coarse_in, west_cin, 1, 2)
    rest_west = send(near_v.at[to_west], near_v.at[from_east], 2, 0)
    rest_east = send(near_v.at[to_east], near_v.at[from_west], 3, 2)

    def rim_copy(slot, t):
        towards = 1 - 2 * lat if one_side else 2 * slot - 1
        other = 0 if one_side else 1 - slot
        return pltpu.make_async_remote_copy(
            src_ref=rim_out.at[slot], dst_ref=rim_in.at[other, 2 - t],
            send_sem=rim_send_sem.at[slot, t], recv_sem=rim_recv_sem.at[other, 2 - t],
            device_id=(lax.rem(lon + n_lon - 1 + t, n_lon), lat + towards), device_id_type=MESH,
        )

    def by_slot(do):
        for slot in slots:
            if one_side:
                do(slot)
            else:
                pl.when(has[slot])(functools.partial(do, slot))

    def rims_start(slot):
        ahead = lax.rem(lon, 2)
        for t in (1 + ahead, 2 - ahead, 0):
            rim_copy(slot, t).start()

    def rims_arrive(slot):
        for t in range(3):
            rim_copy(slot if one_side else 1 - slot, 2 - t).wait_recv()

    def rims_sent(slot):
        for t in range(3):
            rim_copy(slot, t).wait_send()

    loads[0].wait()

    @pl.when(even)
    def _():
        pl.semaphore_wait(barrier, 2)
        coarse_west.start()
        coarse_east.start()

    def columns(source, slot):
        wide_c[slot] = source[...].astype(F32)
        return [wide_c[slot, pl.ds(c, kc, stride=halves), :] for c in range(halves)]

    f_at, i_at = 0, kf * lons
    loads[1].wait()
    wide[f_at:f_at + kf * lons] = fine_in[...].astype(F32)
    loads[2].wait()
    wide[i_at:i_at + nv * lons] = inc_in[...].astype(F32)
    fine_own, inc_own = [], []
    for a in range(lons):
        values = wide[pl.ds(f_at + a, kf, stride=lons), :]
        anom = (values - jnp.mean(values, axis=0, keepdims=True)).astype(BF16)
        vectors = wide[pl.ds(i_at + a, nv, stride=lons), :].astype(BF16)
        near_v[first + a, :kf] = anom
        near_v[first + a, kf:] = vectors
        fine_own.append(anom)
        inc_own.append(vectors)

    @pl.when(even)
    def _():
        rest_west.start()
        rest_east.start()

    coarse_own = columns(coarse_in, 0)
    centred = [v - jnp.mean(v, axis=0, keepdims=True) for v in coarse_own]
    row, lane = iota((kc, lats), 0), iota((kc, lats), 1)
    block = lons * reach
    half = block // 2
    pad = jnp.zeros((kc - halves * kf, lats), F32)
    for slot in slots:
        s = jnp.where(has[0], 0, 1) if one_side else slot

        def strip(values, q):
            return pltpu.roll(values, lax.rem(reach * (s + q), lats), 1)

        cells = jnp.zeros((kc, lats), F32)
        for c in range(halves):
            cells = jnp.where(lane // reach == c, strip(centred[c], c), cells)
        for e in range(halves):
            fine = [fine_own[e + halves * h].astype(F32) for h in range(2)]
            fine = jnp.concatenate(fine + [pad], axis=0)
            cells = jnp.where(lane // reach == halves + e, strip(fine, halves + e), cells)
        cells = cells.T
        low = cells[half:2 * half]
        lane_v = iota((nv, lats), 1)
        for a in range(lons):
            low = jnp.where(
                lane_v // reach == lons + a, strip(inc_own[a].astype(F32), lons + a), low
            )
        rim_out[slot, :half] = cells[:half].astype(BF16)
        rim_out[slot, half:] = low.astype(BF16)

    if not one_side:
        for s in slots:
            @pl.when(jnp.logical_not(has[s]))
            def _():
                rim_in[s] = jnp.zeros(rim_in.shape[1:], BF16)

    one = jnp.int32(1)

    @pl.when(odd)
    def _():
        pl.semaphore_wait(barrier, 2 + 3 * jnp.where(has[0], one, 0) + 3 * jnp.where(has[1], one, 0))
        by_slot(rims_start)
        coarse_west.start()
        coarse_east.start()
        rest_west.start()
        rest_east.start()
        by_side(lambda s: pl.semaphore_signal(
            ok_sem.at[0 if one_side else 1 - s], inc=1, device_id=(lon, lat + 2 * s - 1), device_id_type=MESH
        ))

    loads[3].wait()
    w_coarse = w_ref[1] / (kc - 1)
    fine_ratio = ratio * w_ref[0] / w_ref[1]
    lat_profile = w_coarse * profile(iota((lats, lats), 0) - iota((lats, lats), 1), reach)
    for d in range(lon_reach + 1):
        taper[d] = lat_profile * (1.0 - 0.75 * (d / lon_reach) * (d / lon_reach))

    shape = (half, lats)
    row, lane = iota(shape, 0), iota(shape, 1)
    a_lane, i_lane = lane // (2 * reach), lane % reach
    side = 1 - (lane // reach) % 2
    d_lat = reach + (2 * side - 1) * (row % reach - i_lane)
    for slot in slots:
        mine = side == (jnp.where(has[0], 0, 1) if one_side else slot)
        in_lat = jnp.where(mine, w_coarse * profile(d_lat, reach), 0.0)
        for h in range(2):
            for t in range(3):
                d_lon = (t - 1) * lons + halves * h + row // reach - a_lane
                rim_taper[slot, h, t * half:(t + 1) * half] = in_lat * profile(d_lon, lon_reach)

    def coarse_parts(refined):
        coarse_anom = refined - jnp.mean(refined, axis=0, keepdims=True)
        pair = refined[:kf]
        paired = pair - jnp.mean(pair, axis=0, keepdims=True)
        return coarse_anom.astype(BF16), paired.astype(BF16)

    def set_near(b, refined):
        coarse_anom, paired = coarse_parts(refined)
        near_c[first + b] = coarse_anom
        near_p[first + b] = paired
        return coarse_anom, paired

    def split(scale, values):
        scaled = scale * values.astype(F32)
        high = scaled.astype(BF16).astype(F32)
        return [high, scaled - high]

    def set_own(a, refined):
        coarse_anom, paired = set_near(a, refined)
        rest = split(fine_ratio, near_v[first + a, :kf]) + split(-ratio, paired)
        own_c[a] = coarse_anom.astype(F32).T.astype(BF16)
        own_r[a] = jnp.concatenate(rest, axis=0).T.astype(BF16)

    def own_rows(lo, hi):
        return jnp.concatenate(
            [jnp.concatenate([own_c[a], own_r[a]], axis=1) for a in range(lo, hi)], axis=0
        )

    def members(coarse_anom, fine_anom, paired):
        return jnp.concatenate([coarse_anom, fine_anom, fine_anom, paired, paired], axis=0)

    def near(b):
        at = first + b
        return members(near_c[at], near_v[at, :kf], near_p[at])

    def product(rows, bs, lo, hi):
        gram = jnp.dot(
            own_rows(lo, hi), jnp.concatenate([near(b) for b in bs], axis=1),
            preferred_element_type=F32,
        )
        for n, b in enumerate(bs):
            for a in range(lo, hi):
                part = gram[(a - lo) * lats:(a - lo + 1) * lats, n * lats:(n + 1) * lats]
                rows[a, b] = (part * taper[abs(a - b)]).astype(BF16)

    def apply(rows, a):
        bs = sorted(b for row, b in rows if row == a)
        vectors = jnp.concatenate([near_v[first + b, kf:] for b in bs], axis=1)
        tapered = jnp.concatenate([rows[a, b] for b in bs], axis=1)
        return lax.dot_general(
            vectors, tapered, (((1,), (1,)), ((), ())), preferred_element_type=F32
        )

    def middle(cols, b):
        return cols[b // 2] if b % 2 == 0 else 0.5 * (cols[b // 2] + cols[b // 2 + 1])

    for a in range(lon_reach):
        set_own(a, middle(coarse_own, a))
    rows = {}
    product(rows, tuple(range(lon_reach)), 0, lon_reach)
    for a in range(lon_reach):
        acc[a] = apply(rows, a)

    @pl.when(even)
    def _():
        by_side(lambda s: pl.semaphore_wait(ok_sem.at[0 if one_side else s], 1))
        by_slot(rims_start)

    coarse_west.wait_recv()
    east_c = columns(east_cin, 1)
    set_own(lon_reach, 0.5 * (coarse_own[halves - 1] + east_c[0]))
    rows = {}
    product(rows, tuple(range(lon_reach)), lon_reach, lons)
    product(rows, (lon_reach,), 0, lons)
    for b in range(lon_reach):
        set_near(lons + b, middle(east_c, b))
    for a in range(lon_reach):
        acc[a] += apply(rows, a)
    acc[lon_reach] = apply(rows, lon_reach)
    rest_west.wait_recv()
    rows = {}
    for b in range(0, lon_reach, 2):
        pair = tuple(lons + n for n in range(b, min(b + 2, lon_reach)))
        if len(pair) == 2:
            product(rows, pair[:1], b + 1, b + 2)
        product(rows, pair, b + len(pair), lons)
    for a in range(1, lons):
        acc[a] += apply(rows, a)

    c_rows, r_rows = (
        jnp.concatenate(
            [own[a, at:at + reach] for a in range(lons) for at in (lats - reach, 0)], axis=0
        ).astype(F32)
        for own in (own_c, own_r)
    )
    lead = iota((lats, kc), 1) < kf
    paired = pltpu.roll(r_rows, lats - 2 * kf, 1) + pltpu.roll(r_rows, lats - 3 * kf, 1)
    c_rows += jnp.where(lead, paired, 0.0)
    fine_rows = jnp.where(lead, r_rows, 0.0)
    for h in range(2):
        own_rim[h, :, :kc] = c_rows.astype(BF16)
        own_rim[h, :, kc:] = (pltpu.roll(fine_rows, kf, 1) if h else fine_rows).astype(BF16)

    coarse_east.wait_recv()
    west_c = columns(west_cin, 2)
    west_c.append(coarse_own[0])
    for b in range(1, lons):
        set_near(b - lons, middle(west_c, b))

    def average(x, y):
        return (0.5 * (x.astype(F32) + y.astype(F32))).astype(BF16)

    def rim_edge(slot):
        cells = ([], [])
        for t in range(3):
            west, east = rim_in[slot, t, :reach], rim_in[slot, t, reach:half]
            beyond = rim_in[slot, min(t + 1, 2), :reach]
            for h, pair in enumerate(((west, east), (east, beyond))):
                coarse = jnp.concatenate([pair[0], average(*pair)], axis=0)
                cells[h].append(jnp.concatenate([coarse, rim_in[slot, t, half:]], axis=1))
        taps = []
        for h in range(2):
            gram = lax.dot_general(
                jnp.concatenate(cells[h], axis=0), own_rim[h], (((1,), (1,)), ((), ())),
                preferred_element_type=F32,
            )
            taps.append((gram * rim_taper[slot, h]).astype(BF16))
        order = [taps[h][t * half:(t + 1) * half] for t in range(3) for h in range(2)]
        order.append(jnp.zeros((block, lats), BF16))
        vectors = [rim_in[slot, t, half:].astype(F32) for t in range(3)]
        lane = iota((nv, lats), 1)
        first_two = jnp.where(lane < block, pltpu.roll(vectors[0], block, 1), vectors[1])
        vectors = jnp.concatenate([first_two, pltpu.roll(vectors[2], block, 1)], axis=1)
        return jnp.dot(
            vectors.astype(BF16), jnp.concatenate(order, axis=0), preferred_element_type=F32
        )

    rest_east.wait_recv()
    by_slot(rims_arrive)
    rows = {}
    for b in range(lons - 1, 0, -2):
        pair = tuple(n - lons for n in range(b, max(b - 2, 0), -1))
        product(rows, pair, 0, b + 1 - len(pair))
        if len(pair) == 2:
            product(rows, pair[:1], b - 1, b)
    total = [acc[a] + apply(rows, a) for a in range(lon_reach)] + [acc[lon_reach]]
    edge = functools.reduce(jnp.add, [rim_edge(slot) for slot in slots])
    lane = iota((nv, lats), 1)
    at_edge = (lane < reach) | (lane >= lats - reach)
    for a in range(lons):
        rim = pltpu.roll(edge, (lats - reach - 2 * reach * a) % lats, 1)
        out_ref[pl.ds(a, nv, stride=lons), :] = total[a] + jnp.where(at_edge, rim, 0.0)

    for copy in (coarse_west, coarse_east, rest_west, rest_east):
        copy.wait_send()
    by_slot(rims_sent)


def solution(mesh):
    n_lon, n_lat = mesh.shape["lon"], mesh.shape["lat"]

    def per_device(fine, coarse, inc, weights):
        kf, lons, lats = fine.shape
        kc, halves, _ = coarse.shape
        nv = inc.shape[0]
        near_lons = 3 * lons - 2
        slots = 1 if n_lat == 2 else 2
        assert lons == 4 and nv == kf and lats == kc == 4 * kf
        result = pl.pallas_call(
            functools.partial(kernel, (n_lon, n_lat, kf, kc, nv, lons, lats)),
            out_shape=pltpu.VMEM((nv * lons, lats), F32),
            in_specs=[pl.BlockSpec(memory_space=pl.ANY)] * 4,
            out_specs=pl.BlockSpec(memory_space=pltpu.VMEM),
            scratch_shapes=[
                pltpu.SMEM(weights.shape, F32),
                pltpu.VMEM((kf * lons, lats), BF16),
                pltpu.VMEM((kc * halves, lats), BF16),
                pltpu.VMEM((nv * lons, lats), BF16),
                pltpu.VMEM(((kf + nv) * lons, lats), F32),
                pltpu.VMEM((3, kc * halves, lats), F32),
                pltpu.VMEM((kc * halves, lats), BF16),
                pltpu.VMEM((kc * halves, lats), BF16),
                pltpu.VMEM((slots, 2 * kf, lats), BF16),
                pltpu.VMEM((slots, 3, 2 * kf, lats), BF16),
                pltpu.VMEM((near_lons, kf + nv, lats), BF16),
                pltpu.VMEM((near_lons, kc, lats), BF16),
                pltpu.VMEM((near_lons, kf, lats), BF16),
                pltpu.VMEM((lons, lats, kc), BF16),
                pltpu.VMEM((lons, lats, 4 * kf), BF16),
                pltpu.VMEM((lons, lats, lats), F32),
                pltpu.VMEM((slots, 2, 3 * kf, lats), F32),
                pltpu.VMEM((2, lats, 2 * lats), BF16),
                pltpu.VMEM((lons, nv, lats), F32),
                pltpu.SemaphoreType.DMA((4,)),
                pltpu.SemaphoreType.DMA((4,)),
                pltpu.SemaphoreType.DMA((4,)),
                pltpu.SemaphoreType.DMA((slots, 3)),
                pltpu.SemaphoreType.DMA((slots, 3)),
                pltpu.SemaphoreType.REGULAR((slots,)),
            ],
            compiler_params=pltpu.CompilerParams(collective_id=0, has_side_effects=True),
            name="covariance",
        )(
            weights,
            fine.reshape(kf * lons, lats),
            coarse.reshape(kc * halves, lats),
            inc.reshape(nv * lons, lats),
        )
        return result.reshape(nv, lons, lats)

    spec = P(None, "lon", "lat")
    return jax.shard_map(
        per_device, mesh=mesh, in_specs=(spec, spec, spec, P()), out_specs=spec, check_vma=False
    )
```

```python
import functools

import jax
import jax.numpy as jnp
from jax import lax
from jax.experimental import pallas as pl
from jax.experimental.pallas import tpu as pltpu
from jax.sharding import PartitionSpec as P

MESH = pl.DeviceIdType.MESH
F32, BF16 = jnp.float32, jnp.bfloat16


def profile(distance, extent):
    ratio = distance.astype(F32) / extent
    return jnp.where(jnp.abs(distance) <= extent, 1.0 - 0.75 * ratio * ratio, 0.0)


def iota(shape, dim):
    return lax.broadcasted_iota(jnp.int32, shape, dim)


def kernel(
    sizes, weights_ref, fine_ref, coarse_ref, inc_ref, out_ref,
    w_ref, fine_in, coarse_in, inc_in, wide, wide_c, west_cin, east_cin, rim_out, rim_in,
    near_v, near_c, near_p, own_c, own_r, taper, rim_taper, own_rim, acc,
    in_sem, send_sem, recv_sem, rim_send_sem, rim_recv_sem, ok_sem,
):
    n_lon, n_lat, kf, kc, nv, lons, lats = sizes
    halves, reach, lon_reach = lons // 2, lats // 8, lons - 1
    ratio = (kc - 1) / (kf - 1)
    lon, lat = lax.axis_index("lon"), lax.axis_index("lat")
    sides = (lax.rem(lon + n_lon - 1, n_lon), lon, lax.rem(lon + 1, n_lon))
    has = (lat > 0, lat < n_lat - 1)
    odd = lax.rem(lat, 2) == 1
    even = jnp.logical_not(odd)
    one_side = n_lat == 2
    slots = range(1) if one_side else range(2)

    barrier = pltpu.get_barrier_semaphore()

    loads = [
        pltpu.make_async_copy(src, dst, in_sem.at[n])
        for n, (src, dst) in enumerate(
            ((coarse_ref, coarse_in), (fine_ref, fine_in), (inc_ref, inc_in), (weights_ref, w_ref))
        )
    ]
    for load in loads:
        load.start()

    def by_side(do):
        for s in range(2):
            if not one_side:
                pl.when(has[s])(functools.partial(do, s))
        if one_side:
            do(lax.rem(lat + 1, 2))

    def greet(to_lon, to_lat):
        pl.semaphore_signal(barrier, inc=1, device_id=(to_lon, to_lat), device_id_type=MESH)

    greet(sides[0], lat)
    greet(sides[2], lat)

    @pl.when(even)
    def _():
        by_side(lambda s: [greet(sides[t], lat + 2 * s - 1) for t in (1, 0, 2)] and None)

    def send(src, dst, n, towards):
        return pltpu.make_async_remote_copy(
            src_ref=src, dst_ref=dst, send_sem=send_sem.at[n], recv_sem=recv_sem.at[n],
            device_id=(sides[towards], lat), device_id_type=MESH,
        )

    first, past, last = lon_reach, lon_reach + lons, 2 * lon_reach + lons
    to_west, to_east = pl.ds(first, lon_reach), pl.ds(first + 1, lon_reach)
    from_west, from_east = pl.ds(0, lon_reach), pl.ds(past, lon_reach)
    coarse_west = send(coarse_in, east_cin, 0, 0)
    coarse_east = send(coarse_in, west_cin, 1, 2)
    rest_west = send(near_v.at[to_west], near_v.at[from_east], 2, 0)
    rest_east = send(near_v.at[to_east], near_v.at[from_west], 3, 2)

    def rim_copy(slot, t):
        towards = 1 - 2 * lat if one_side else 2 * slot - 1
        other = 0 if one_side else 1 - slot
        return pltpu.make_async_remote_copy(
            src_ref=rim_out.at[slot], dst_ref=rim_in.at[other, 2 - t],
            send_sem=rim_send_sem.at[slot, t], recv_sem=rim_recv_sem.at[other, 2 - t],
            device_id=(lax.rem(lon + n_lon - 1 + t, n_lon), lat + towards), device_id_type=MESH,
        )

    def by_slot(do):
        for slot in slots:
            if one_side:
                do(slot)
            else:
                pl.when(has[slot])(functools.partial(do, slot))

    def rims_start(slot):
        ahead = lax.rem(lon, 2)
        for t in (1 + ahead, 2 - ahead, 0):
            rim_copy(slot, t).start()

    def rims_arrive(slot):
        for t in range(3):
            rim_copy(slot if one_side else 1 - slot, 2 - t).wait_recv()

    def rims_sent(slot):
        for t in range(3):
            rim_copy(slot, t).wait_send()

    loads[0].wait()

    @pl.when(even)
    def _():
        pl.semaphore_wait(barrier, 2)
        coarse_west.start()
        coarse_east.start()

    def columns(source, slot):
        wide_c[slot] = source[...].astype(F32)
        return [wide_c[slot, pl.ds(c, kc, stride=halves), :] for c in range(halves)]

    f_at, i_at = 0, kf * lons
    loads[1].wait()
    wide[f_at:f_at + kf * lons] = fine_in[...].astype(F32)
    loads[2].wait()
    wide[i_at:i_at + nv * lons] = inc_in[...].astype(F32)
    fine_own, inc_own = [], []
    for a in range(lons):
        values = wide[pl.ds(f_at + a, kf, stride=lons), :]
        anom = (values - jnp.mean(values, axis=0, keepdims=True)).astype(BF16)
        vectors = wide[pl.ds(i_at + a, nv, stride=lons), :].astype(BF16)
        near_v[first + a, :kf] = anom
        near_v[first + a, kf:] = vectors
        fine_own.append(anom)
        inc_own.append(vectors)

    @pl.when(even)
    def _():
        rest_west.start()
        rest_east.start()

    coarse_own = columns(coarse_in, 0)
    centred = [v - jnp.mean(v, axis=0, keepdims=True) for v in coarse_own]
    row, lane = iota((kc, lats), 0), iota((kc, lats), 1)
    block = lons * reach
    half = block // 2
    pad = jnp.zeros((kc - halves * kf, lats), F32)
    for slot in slots:
        s = jnp.where(has[0], 0, 1) if one_side else slot

        def strip(values, q):
            return pltpu.roll(values, lax.rem(reach * (s + q), lats), 1)

        cells = jnp.zeros((kc, lats), F32)
        for c in range(halves):
            cells = jnp.where(lane // reach == c, strip(centred[c], c), cells)
        for e in range(halves):
            fine = [fine_own[e + halves * h].astype(F32) for h in range(2)]
            fine = jnp.concatenate(fine + [pad], axis=0)
            cells = jnp.where(lane // reach == halves + e, strip(fine, halves + e), cells)
        cells = cells.T
        low = cells[half:2 * half]
        lane_v = iota((nv, lats), 1)
        for a in range(lons):
            low = jnp.where(
                lane_v // reach == lons + a, strip(inc_own[a].astype(F32), lons + a), low
            )
        rim_out[slot, :half] = cells[:half].astype(BF16)
        rim_out[slot, half:] = low.astype(BF16)

    if not one_side:
        for s in slots:
            @pl.when(jnp.logical_not(has[s]))
            def _():
                rim_in[s] = jnp.zeros(rim_in.shape[1:], BF16)

    one = jnp.int32(1)

    @pl.when(odd)
    def _():
        pl.semaphore_wait(barrier, 2 + 3 * jnp.where(has[0], one, 0) + 3 * jnp.where(has[1], one, 0))
        by_slot(rims_start)
        coarse_west.start()
        coarse_east.start()
        rest_west.start()
        rest_east.start()
        by_side(lambda s: pl.semaphore_signal(
            ok_sem.at[0 if one_side else 1 - s], inc=1, device_id=(lon, lat + 2 * s - 1), device_id_type=MESH
        ))

    loads[3].wait()
    w_coarse = w_ref[1] / (kc - 1)
    fine_ratio = ratio * w_ref[0] / w_ref[1]
    lat_profile = w_coarse * profile(iota((lats, lats), 0) - iota((lats, lats), 1), reach)
    for d in range(lon_reach + 1):
        taper[d] = lat_profile * (1.0 - 0.75 * (d / lon_reach) * (d / lon_reach))

    shape = (half, lats)
    row, lane = iota(shape, 0), iota(shape, 1)
    a_lane, i_lane = lane // (2 * reach), lane % reach
    side = 1 - (lane // reach) % 2
    d_lat = reach + (2 * side - 1) * (row % reach - i_lane)
    for slot in slots:
        mine = side == (jnp.where(has[0], 0, 1) if one_side else slot)
        in_lat = jnp.where(mine, w_coarse * profile(d_lat, reach), 0.0)
        for h in range(2):
            for t in range(3):
                d_lon = (t - 1) * lons + halves * h + row // reach - a_lane
                rim_taper[slot, h, t * half:(t + 1) * half] = in_lat * profile(d_lon, lon_reach)

    def coarse_parts(refined):
        coarse_anom = refined - jnp.mean(refined, axis=0, keepdims=True)
        pair = refined[:kf]
        paired = pair - jnp.mean(pair, axis=0, keepdims=True)
        return coarse_anom.astype(BF16), paired.astype(BF16)

    def set_near(b, refined):
        coarse_anom, paired = coarse_parts(refined)
        near_c[first + b] = coarse_anom
        near_p[first + b] = paired
        return coarse_anom, paired

    def split(scale, values):
        scaled = scale * values.astype(F32)
        high = scaled.astype(BF16).astype(F32)
        return [high, scaled - high]

    def set_own(a, refined):
        coarse_anom, paired = set_near(a, refined)
        rest = split(fine_ratio, near_v[first + a, :kf]) + split(-ratio, paired)
        own_c[a] = coarse_anom.astype(F32).T.astype(BF16)
        own_r[a] = jnp.concatenate(rest, axis=0).T.astype(BF16)

    def own_rows(lo, hi):
        return jnp.concatenate(
            [jnp.concatenate([own_c[a], own_r[a]], axis=1) for a in range(lo, hi)], axis=0
        )

    def members(coarse_anom, fine_anom, paired):
        return jnp.concatenate([coarse_anom, fine_anom, fine_anom, paired, paired], axis=0)

    def near(b):
        at = first + b
        return members(near_c[at], near_v[at, :kf], near_p[at])

    def product(rows, bs, lo, hi):
        gram = jnp.dot(
            own_rows(lo, hi), jnp.concatenate([near(b) for b in bs], axis=1),
            preferred_element_type=F32,
        )
        for n, b in enumerate(bs):
            for a in range(lo, hi):
                part = gram[(a - lo) * lats:(a - lo + 1) * lats, n * lats:(n + 1) * lats]
                rows[a, b] = (part * taper[abs(a - b)]).astype(BF16)

    def apply(rows, a):
        bs = sorted(b for row, b in rows if row == a)
        vectors = jnp.concatenate([near_v[first + b, kf:] for b in bs], axis=1)
        tapered = jnp.concatenate([rows[a, b] for b in bs], axis=1)
        return lax.dot_general(
            vectors, tapered, (((1,), (1,)), ((), ())), preferred_element_type=F32
        )

    def middle(cols, b):
        return cols[b // 2] if b % 2 == 0 else 0.5 * (cols[b // 2] + cols[b // 2 + 1])

    for a in range(lon_reach):
        set_own(a, middle(coarse_own, a))
    rows = {}
    product(rows, tuple(range(lon_reach)), 0, lon_reach)
    for a in range(lon_reach):
        acc[a] = apply(rows, a)

    @pl.when(even)
    def _():
        by_side(lambda s: pl.semaphore_wait(ok_sem.at[0 if one_side else s], 1))
        by_slot(rims_start)

    coarse_west.wait_recv()
    east_c = columns(east_cin, 1)
    set_own(lon_reach, 0.5 * (coarse_own[halves - 1] + east_c[0]))
    rows = {}
    product(rows, tuple(range(lon_reach)), lon_reach, lons)
    product(rows, (lon_reach,), 0, lons)
    for b in range(lon_reach):
        set_near(lons + b, middle(east_c, b))
    for a in range(lon_reach):
        acc[a] += apply(rows, a)
    acc[lon_reach] = apply(rows, lon_reach)
    rest_west.wait_recv()
    rows = {}
    for b in range(0, lon_reach, 2):
        pair = tuple(lons + n for n in range(b, min(b + 2, lon_reach)))
        if len(pair) == 2:
            product(rows, pair[:1], b + 1, b + 2)
        product(rows, pair, b + len(pair), lons)
    for a in range(1, lons):
        acc[a] += apply(rows, a)

    c_rows, r_rows = (
        jnp.concatenate(
            [own[a, at:at + reach] for a in range(lons) for at in (lats - reach, 0)], axis=0
        ).astype(F32)
        for own in (own_c, own_r)
    )
    lead = iota((lats, kc), 1) < kf
    paired = pltpu.roll(r_rows, lats - 2 * kf, 1) + pltpu.roll(r_rows, lats - 3 * kf, 1)
    c_rows += jnp.where(lead, paired, 0.0)
    fine_rows = jnp.where(lead, r_rows, 0.0)
    for h in range(2):
        own_rim[h, :, :kc] = c_rows.astype(BF16)
        own_rim[h, :, kc:] = (pltpu.roll(fine_rows, kf, 1) if h else fine_rows).astype(BF16)

    coarse_east.wait_recv()
    west_c = columns(west_cin, 2)
    west_c.append(coarse_own[0])
    for b in range(1, lons):
        set_near(b - lons, middle(west_c, b))

    def average(x, y):
        return (0.5 * (x.astype(F32) + y.astype(F32))).astype(BF16)

    def rim_taps(slot):
        cells = ([], [])
        for t in range(3):
            west, east = rim_in[slot, t, :reach], rim_in[slot, t, reach:half]
            beyond = rim_in[slot, min(t + 1, 2), :reach]
            for h, pair in enumerate(((west, east), (east, beyond))):
                coarse = jnp.concatenate([pair[0], average(*pair)], axis=0)
                cells[h].append(jnp.concatenate([coarse, rim_in[slot, t, half:]], axis=1))
        taps = []
        for h in range(2):
            gram = lax.dot_general(
                jnp.concatenate(cells[h], axis=0), own_rim[h], (((1,), (1,)), ((), ())),
                preferred_element_type=F32,
            )
            taps.append((gram * rim_taper[slot, h]).astype(BF16))
        return taps

    def rim_edge(slot, taps):
        order = [taps[h][t * half:(t + 1) * half] for t in range(3) for h in range(2)]
        order.append(jnp.zeros((block, lats), BF16))
        vectors = [rim_in[slot, t, half:].astype(F32) for t in range(3)]
        lane = iota((nv, lats), 1)
        first_two = jnp.where(lane < block, pltpu.roll(vectors[0], block, 1), vectors[1])
        vectors = jnp.concatenate([first_two, pltpu.roll(vectors[2], block, 1)], axis=1)
        return jnp.dot(
            vectors.astype(BF16), jnp.concatenate(order, axis=0), preferred_element_type=F32
        )

    rest_east.wait_recv()
    by_slot(rims_arrive)
    taps = [rim_taps(slot) for slot in slots]
    rows = {}
    for b in range(lons - 1, 0, -2):
        pair = tuple(n - lons for n in range(b, max(b - 2, 0), -1))
        product(rows, pair, 0, b + 1 - len(pair))
        if len(pair) == 2:
            product(rows, pair[:1], b - 1, b)
    edge = functools.reduce(jnp.add, [rim_edge(slot, taps[slot]) for slot in slots])
    total = [acc[a] + apply(rows, a) for a in range(lon_reach)] + [acc[lon_reach]]
    lane = iota((nv, lats), 1)
    at_edge = (lane < reach) | (lane >= lats - reach)
    for a in range(lons):
        rim = pltpu.roll(edge, (lats - reach - 2 * reach * a) % lats, 1)
        out_ref[pl.ds(a, nv, stride=lons), :] = total[a] + jnp.where(at_edge, rim, 0.0)

    for copy in (coarse_west, coarse_east, rest_west, rest_east):
        copy.wait_send()
    by_slot(rims_sent)


def solution(mesh):
    n_lon, n_lat = mesh.shape["lon"], mesh.shape["lat"]

    def per_device(fine, coarse, inc, weights):
        kf, lons, lats = fine.shape
        kc, halves, _ = coarse.shape
        nv = inc.shape[0]
        near_lons = 3 * lons - 2
        slots = 1 if n_lat == 2 else 2
        assert lons == 4 and nv == kf and lats == kc == 4 * kf
        result = pl.pallas_call(
            functools.partial(kernel, (n_lon, n_lat, kf, kc, nv, lons, lats)),
            out_shape=pltpu.VMEM((nv * lons, lats), F32),
            in_specs=[pl.BlockSpec(memory_space=pl.ANY)] * 4,
            out_specs=pl.BlockSpec(memory_space=pltpu.VMEM),
            scratch_shapes=[
                pltpu.SMEM(weights.shape, F32),
                pltpu.VMEM((kf * lons, lats), BF16),
                pltpu.VMEM((kc * halves, lats), BF16),
                pltpu.VMEM((nv * lons, lats), BF16),
                pltpu.VMEM(((kf + nv) * lons, lats), F32),
                pltpu.VMEM((3, kc * halves, lats), F32),
                pltpu.VMEM((kc * halves, lats), BF16),
                pltpu.VMEM((kc * halves, lats), BF16),
                pltpu.VMEM((slots, 2 * kf, lats), BF16),
                pltpu.VMEM((slots, 3, 2 * kf, lats), BF16),
                pltpu.VMEM((near_lons, kf + nv, lats), BF16),
                pltpu.VMEM((near_lons, kc, lats), BF16),
                pltpu.VMEM((near_lons, kf, lats), BF16),
                pltpu.VMEM((lons, lats, kc), BF16),
                pltpu.VMEM((lons, lats, 4 * kf), BF16),
                pltpu.VMEM((lons, lats, lats), F32),
                pltpu.VMEM((slots, 2, 3 * kf, lats), F32),
                pltpu.VMEM((2, lats, 2 * lats), BF16),
                pltpu.VMEM((lons, nv, lats), F32),
                pltpu.SemaphoreType.DMA((4,)),
                pltpu.SemaphoreType.DMA((4,)),
                pltpu.SemaphoreType.DMA((4,)),
                pltpu.SemaphoreType.DMA((slots, 3)),
                pltpu.SemaphoreType.DMA((slots, 3)),
                pltpu.SemaphoreType.REGULAR((slots,)),
            ],
            compiler_params=pltpu.CompilerParams(collective_id=0, has_side_effects=True),
            name="covariance",
        )(
            weights,
            fine.reshape(kf * lons, lats),
            coarse.reshape(kc * halves, lats),
            inc.reshape(nv * lons, lats),
        )
        return result.reshape(nv, lons, lats)

    spec = P(None, "lon", "lat")
    return jax.shard_map(
        per_device, mesh=mesh, in_specs=(spec, spec, spec, P()), out_specs=spec, check_vma=False
    )
```

```python
import functools

import jax
import jax.numpy as jnp
from jax import lax
from jax.experimental import pallas as pl
from jax.experimental.pallas import tpu as pltpu
from jax.sharding import PartitionSpec as P

MESH = pl.DeviceIdType.MESH
F32, BF16 = jnp.float32, jnp.bfloat16


def profile(distance, extent):
    ratio = distance.astype(F32) / extent
    return jnp.where(jnp.abs(distance) <= extent, 1.0 - 0.75 * ratio * ratio, 0.0)


def iota(shape, dim):
    return lax.broadcasted_iota(jnp.int32, shape, dim)


def kernel(
    sizes, weights_ref, fine_ref, coarse_ref, inc_ref, out_ref,
    w_ref, fine_in, coarse_in, inc_in, wide, wide_c, west_cin, east_cin, turned, rim_in,
    near_f, near_i, near_c, near_p, own_c, own_r, taper, rim_taper, own_rim, acc,
    in_sem, send_sem, recv_sem, rim_send_sem, rim_recv_sem, ok_sem,
):
    n_lon, n_lat, kf, kc, nv, lons, lats = sizes
    halves, reach, lon_reach = lons // 2, lats // 8, lons - 1
    ratio = (kc - 1) / (kf - 1)
    lon, lat = lax.axis_index("lon"), lax.axis_index("lat")
    sides = (lax.rem(lon + n_lon - 1, n_lon), lon, lax.rem(lon + 1, n_lon))
    has = (lat > 0, lat < n_lat - 1)
    odd = lax.rem(lat, 2) == 1
    even = jnp.logical_not(odd)
    one_side = n_lat == 2
    slots = range(1) if one_side else range(2)

    barrier = pltpu.get_barrier_semaphore()

    loads = [
        pltpu.make_async_copy(src, dst, in_sem.at[n])
        for n, (src, dst) in enumerate(
            ((coarse_ref, coarse_in), (fine_ref, fine_in), (inc_ref, inc_in), (weights_ref, w_ref))
        )
    ]
    for load in loads:
        load.start()

    def by_side(do):
        for s in range(2):
            if not one_side:
                pl.when(has[s])(functools.partial(do, s))
        if one_side:
            do(lax.rem(lat + 1, 2))

    def greet(to_lon, to_lat):
        pl.semaphore_signal(barrier, inc=1, device_id=(to_lon, to_lat), device_id_type=MESH)

    greet(sides[0], lat)
    greet(sides[2], lat)

    @pl.when(even)
    def _():
        by_side(lambda s: [greet(sides[t], lat + 2 * s - 1) for t in (1, 0, 2)] and None)

    def send(src, dst, sent, arrived, towards):
        return pltpu.make_async_remote_copy(
            src_ref=src, dst_ref=dst, send_sem=send_sem.at[sent], recv_sem=recv_sem.at[arrived],
            device_id=(sides[towards], lat), device_id_type=MESH,
        )

    first, past, last = lon_reach, lon_reach + lons, 2 * lon_reach + lons
    to_west, to_east = pl.ds(first, lon_reach), pl.ds(first + 1, lon_reach)
    from_west, from_east = pl.ds(0, lon_reach), pl.ds(past, lon_reach)
    coarse_west = send(coarse_in, east_cin, 0, 0, 0)
    coarse_east = send(coarse_in, west_cin, 0, 1, 2)
    fine_west = send(near_f.at[to_west], near_f.at[from_east], 1, 2, 0)
    fine_east = send(near_f.at[to_east], near_f.at[from_west], 1, 3, 2)
    inc_west = send(near_i.at[to_west], near_i.at[from_east], 1, 2, 0)
    inc_east = send(near_i.at[to_east], near_i.at[from_west], 1, 4, 2)

    def rim_copy(slot, t):
        towards = 1 - 2 * lat if one_side else 2 * slot - 1
        other = 0 if one_side else 1 - slot
        at = jnp.where(has[0], 0, lats - reach) if one_side else slot * (lats - reach)
        return pltpu.make_async_remote_copy(
            src_ref=turned.at[:, pl.ds(pl.multiple_of(at, reach), reach)], dst_ref=rim_in.at[other, 2 - t],
            send_sem=rim_send_sem.at[slot], recv_sem=rim_recv_sem.at[other],
            device_id=(lax.rem(lon + n_lon - 1 + t, n_lon), lat + towards), device_id_type=MESH,
        )

    def by_slot(do):
        for slot in slots:
            if one_side:
                do(slot)
            else:
                pl.when(has[slot])(functools.partial(do, slot))

    def rims_start(slot):
        ahead = lax.rem(lon, 2)
        for t in (1 + ahead, 2 - ahead, 0):
            rim_copy(slot, t).start()

    def drain(ref, sem):
        pltpu.make_async_copy(ref, ref, sem).wait()

    def rims_arrive(slot):
        drain(rim_in.at[slot], rim_recv_sem.at[slot])

    def rims_sent(slot):
        drain(rim_in.at[slot], rim_send_sem.at[slot])

    loads[0].wait()

    @pl.when(even)
    def _():
        pl.semaphore_wait(barrier, 2)
        coarse_west.start()
        coarse_east.start()

    def columns(source, slot):
        wide_c[slot] = source[...].astype(F32)
        return [wide_c[slot, pl.ds(c, kc, stride=halves), :] for c in range(halves)]

    f_at, i_at = 0, kf * lons
    loads[1].wait()
    loads[2].wait()
    coarse_own = columns(coarse_in, 0)
    wide[f_at:f_at + kf * lons] = fine_in[...].astype(F32)
    wide[i_at:i_at + nv * lons] = inc_in[...].astype(F32)
    centred = [v - jnp.mean(v, axis=0, keepdims=True) for v in coarse_own]
    fine_own, inc_own = [], []
    for a in range(lons):
        values = wide[pl.ds(f_at + a, kf, stride=lons), :]
        anom = (values - jnp.mean(values, axis=0, keepdims=True)).astype(BF16)
        vectors = wide[pl.ds(i_at + a, nv, stride=lons), :].astype(BF16)
        near_f[first + a] = anom
        near_i[first + a] = vectors
        fine_own.append(anom)
        inc_own.append(vectors)
    stacks = centred + [
        jnp.concatenate([v.astype(F32) for v in own], axis=0) for own in (fine_own, inc_own)
    ]
    for n, stack in enumerate(stacks):
        turned[n] = stack.T.astype(BF16)

    @pl.when(even)
    def _():
        fine_west.start()
        fine_east.start()
        inc_west.start()
        inc_east.start()

    if not one_side:
        for s in slots:
            @pl.when(jnp.logical_not(has[s]))
            def _():
                rim_in[s] = jnp.zeros(rim_in.shape[1:], BF16)

    one = jnp.int32(1)

    @pl.when(odd)
    def _():
        pl.semaphore_wait(barrier, 2 + 3 * jnp.where(has[0], one, 0) + 3 * jnp.where(has[1], one, 0))
        by_slot(rims_start)
        coarse_west.start()
        coarse_east.start()
        fine_west.start()
        fine_east.start()
        inc_west.start()
        inc_east.start()
        by_side(lambda s: pl.semaphore_signal(
            ok_sem.at[0 if one_side else 1 - s], inc=1, device_id=(lon, lat + 2 * s - 1), device_id_type=MESH
        ))

    loads[3].wait()
    w_coarse = w_ref[1] / (kc - 1)
    fine_ratio = ratio * w_ref[0] / w_ref[1]
    lat_profile = w_coarse * profile(iota((lats, lats), 0) - iota((lats, lats), 1), reach)
    for d in range(lon_reach + 1):
        taper[d] = lat_profile * (1.0 - 0.75 * (d / lon_reach) * (d / lon_reach))

    shape = (3 * reach, lats)
    row, lane = iota(shape, 0), iota(shape, 1)
    a_lane, i_lane = lane // (2 * reach), lane % reach
    side = 1 - (lane // reach) % 2
    d_lat = reach + (2 * side - 1) * (row % reach - i_lane)
    for slot in slots:
        mine = side == (jnp.where(has[0], 0, 1) if one_side else slot)
        in_lat = jnp.where(mine, w_coarse * profile(d_lat, reach), 0.0)
        for b in range(lons):
            d_lon = (row // reach - 1) * lons + b - a_lane
            rim_taper[slot, b] = in_lat * profile(d_lon, lon_reach)

    def coarse_parts(refined):
        coarse_anom = refined - jnp.mean(refined, axis=0, keepdims=True)
        pair = refined[:kf]
        paired = pair - jnp.mean(pair, axis=0, keepdims=True)
        return coarse_anom.astype(BF16), paired.astype(BF16)

    def set_near(b, refined):
        coarse_anom, paired = coarse_parts(refined)
        near_c[first + b] = coarse_anom
        near_p[first + b] = paired
        return coarse_anom, paired

    def split(scale, values):
        scaled = scale * values.astype(F32)
        high = scaled.astype(BF16).astype(F32)
        return [high, scaled - high]

    def set_own(a, refined):
        coarse_anom, paired = set_near(a, refined)
        if a % 2 == 0:
            own_c[a] = turned[a // 2]
        else:
            own_c[a] = coarse_anom.astype(F32).T.astype(BF16)
        rest = split(fine_ratio, near_f[first + a]) + split(-ratio, paired)
        own_r[a] = jnp.concatenate(rest, axis=0).T.astype(BF16)

    def own_rows(lo, hi):
        return jnp.concatenate(
            [jnp.concatenate([own_c[a], own_r[a]], axis=1) for a in range(lo, hi)], axis=0
        )

    def members(coarse_anom, fine_anom, paired):
        return jnp.concatenate([coarse_anom, fine_anom, fine_anom, paired, paired], axis=0)

    def near(b):
        at = first + b
        return members(near_c[at], near_f[at], near_p[at])

    def product(rows, bs, lo, hi):
        gram = jnp.dot(
            own_rows(lo, hi), jnp.concatenate([near(b) for b in bs], axis=1),
            preferred_element_type=F32,
        )
        for n, b in enumerate(bs):
            for a in range(lo, hi):
                part = gram[(a - lo) * lats:(a - lo + 1) * lats, n * lats:(n + 1) * lats]
                rows[a, b] = (part * taper[abs(a - b)]).astype(BF16)

    def apply(rows, a):
        bs = sorted(b for row, b in rows if row == a)
        vectors = jnp.concatenate([near_i[first + b] for b in bs], axis=1)
        tapered = jnp.concatenate([rows[a, b] for b in bs], axis=1)
        return lax.dot_general(
            vectors, tapered, (((1,), (1,)), ((), ())), preferred_element_type=F32
        )

    def middle(cols, b):
        return cols[b // 2] if b % 2 == 0 else 0.5 * (cols[b // 2] + cols[b // 2 + 1])

    for a in range(lon_reach):
        set_own(a, middle(coarse_own, a))
    rows = {}
    product(rows, tuple(range(lon_reach)), 0, lon_reach)
    for a in range(lon_reach):
        acc[a] = apply(rows, a)

    @pl.when(even)
    def _():
        by_side(lambda s: pl.semaphore_wait(ok_sem.at[0 if one_side else s], 1))
        by_slot(rims_start)

    coarse_west.wait_recv()
    east_c = columns(east_cin, 1)
    set_own(lon_reach, 0.5 * (coarse_own[halves - 1] + east_c[0]))
    rows = {}
    product(rows, tuple(range(lon_reach)), lon_reach, lons)
    product(rows, (lon_reach,), 0, lons)
    for b in range(lon_reach):
        set_near(lons + b, middle(east_c, b))
    for a in range(lon_reach):
        acc[a] += apply(rows, a)
    acc[lon_reach] = apply(rows, lon_reach)
    drain(near_f.at[pl.ds(0, 2 * lon_reach)], recv_sem.at[2])
    rows = {}
    for b in range(0, lon_reach, 2):
        pair = tuple(lons + n for n in range(b, min(b + 2, lon_reach)))
        if len(pair) == 2:
            product(rows, pair[:1], b + 1, b + 2)
        product(rows, pair, b + len(pair), lons)
    for a in range(1, lons):
        acc[a] += apply(rows, a)

    c_rows, r_rows = (
        jnp.concatenate(
            [own[a, at:at + reach] for a in range(lons) for at in (lats - reach, 0)], axis=0
        ).astype(F32)
        for own in (own_c, own_r)
    )
    lead = iota((lats, kc), 1) < kf
    paired = pltpu.roll(r_rows, lats - 2 * kf, 1) + pltpu.roll(r_rows, lats - 3 * kf, 1)
    c_rows += jnp.where(lead, paired, 0.0)
    fine_rows = jnp.where(lead, r_rows, 0.0)
    fine_rows += pltpu.roll(fine_rows, kf, 1)
    fine_rows += pltpu.roll(fine_rows, 2 * kf, 1)
    own_rim[:, :kc] = c_rows.astype(BF16)
    own_rim[:, kc:] = fine_rows.astype(BF16)

    coarse_east.wait_recv()
    west_c = columns(west_cin, 2)
    west_c.append(coarse_own[0])
    for b in range(1, lons):
        set_near(b - lons, middle(west_c, b))

    def average(x, y):
        return (0.5 * (x.astype(F32) + y.astype(F32))).astype(BF16)

    def rim_taps(slot):
        group = iota((reach, lats), 1) // kf
        taps = []
        for pair in range(0, lons, 2):
            cells = []
            for b in (pair, pair + 1):
                for t in range(3):
                    cols = [rim_in[slot, t, c] for c in range(halves)]
                    cols.append(rim_in[slot, min(t + 1, 2), 0])
                    coarse = cols[b // 2] if b % 2 == 0 else average(cols[b // 2], cols[b // 2 + 1])
                    fine = jnp.where(group == b, rim_in[slot, t, halves].astype(F32), 0.0)
                    cells.append(jnp.concatenate([coarse, fine.astype(BF16)], axis=1))
            gram = lax.dot_general(
                jnp.concatenate(cells, axis=0), own_rim[...], (((1,), (1,)), ((), ())),
                preferred_element_type=F32,
            )
            for e in range(2):
                part = gram[3 * reach * e:3 * reach * (e + 1)]
                taps.append((part * rim_taper[slot, pair + e]).astype(BF16))
                taps.append(jnp.zeros((reach, lats), BF16))
        return jnp.concatenate(taps, axis=0)

    def rim_vectors(slot):
        cells = [rim_in[slot, t, halves + 1].astype(F32) for t in range(3)]
        cells = (cells + [jnp.zeros((reach, lats), F32)]) * 2
        cells = jnp.concatenate(cells, axis=0).T
        lower = iota((nv, lats), 1) < lats // 2
        pairs = [
            jnp.where(lower, cells[b * nv:(b + 1) * nv], cells[(b + 1) * nv:(b + 2) * nv])
            for b in range(0, lons, 2)
        ]
        return jnp.concatenate(pairs, axis=1).astype(BF16)

    drain(wide_c.at[0], send_sem.at[0])
    drain(turned.at[pl.ds(0, 3)], send_sem.at[1])
    fine_east.wait_recv()
    rows = {}
    for b in range(lons - 1, 0, -2):
        pair = tuple(n - lons for n in range(b, max(b - 2, 0), -1))
        product(rows, pair, 0, b + 1 - len(pair))
        if len(pair) == 2:
            product(rows, pair[:1], b - 1, b)
    inc_east.wait_recv()
    by_slot(rims_arrive)
    vectors = [rim_vectors(slot) for slot in slots]
    taps = [rim_taps(slot) for slot in slots]
    edge = functools.reduce(
        jnp.add,
        [
            jnp.dot(
                vectors[slot][:, at:at + lats], taps[slot][at:at + lats],
                preferred_element_type=F32,
            )
            for slot in slots
            for at in (0, lats)
        ],
    )
    total = [acc[a] + apply(rows, a) for a in range(lon_reach)] + [acc[lon_reach]]
    lane = iota((nv, lats), 1)
    at_edge = (lane < reach) | (lane >= lats - reach)
    for a in range(lons):
        rim = pltpu.roll(edge, (lats - reach - 2 * reach * a) % lats, 1)
        out_ref[pl.ds(a, nv, stride=lons), :] = total[a] + jnp.where(at_edge, rim, 0.0)

    by_slot(rims_sent)


def solution(mesh):
    n_lon, n_lat = mesh.shape["lon"], mesh.shape["lat"]

    def per_device(fine, coarse, inc, weights):
        kf, lons, lats = fine.shape
        kc, halves, _ = coarse.shape
        nv = inc.shape[0]
        near_lons = 3 * lons - 2
        slots = 1 if n_lat == 2 else 2
        assert lons == 4 and nv == kf and lats == kc == 4 * kf
        result = pl.pallas_call(
            functools.partial(kernel, (n_lon, n_lat, kf, kc, nv, lons, lats)),
            out_shape=pltpu.VMEM((nv * lons, lats), F32),
            in_specs=[pl.BlockSpec(memory_space=pl.ANY)] * 4,
            out_specs=pl.BlockSpec(memory_space=pltpu.VMEM),
            scratch_shapes=[
                pltpu.SMEM(weights.shape, F32),
                pltpu.VMEM((kf * lons, lats), BF16),
                pltpu.VMEM((kc * halves, lats), BF16),
                pltpu.VMEM((nv * lons, lats), BF16),
                pltpu.VMEM(((kf + nv) * lons, lats), F32),
                pltpu.VMEM((3, kc * halves, lats), F32),
                pltpu.VMEM((kc * halves, lats), BF16),
                pltpu.VMEM((kc * halves, lats), BF16),
                pltpu.VMEM((halves + 2, lats, kc), BF16),
                pltpu.VMEM((slots, 3, halves + 2, lats // 8, kc), BF16),
                pltpu.VMEM((near_lons, kf, lats), BF16),
                pltpu.VMEM((near_lons, nv, lats), BF16),
                pltpu.VMEM((near_lons, kc, lats), BF16),
                pltpu.VMEM((near_lons, kf, lats), BF16),
                pltpu.VMEM((lons, lats, kc), BF16),
                pltpu.VMEM((lons, lats, 4 * kf), BF16),
                pltpu.VMEM((lons, lats, lats), F32),
                pltpu.VMEM((slots, lons, 3 * lats // 8, lats), F32),
                pltpu.VMEM((lats, 2 * lats), BF16),
                pltpu.VMEM((lons, nv, lats), F32),
                pltpu.SemaphoreType.DMA((4,)),
                pltpu.SemaphoreType.DMA((2,)),
                pltpu.SemaphoreType.DMA((5,)),
                pltpu.SemaphoreType.DMA((slots,)),
                pltpu.SemaphoreType.DMA((slots,)),
                pltpu.SemaphoreType.REGULAR((slots,)),
            ],
            compiler_params=pltpu.CompilerParams(collective_id=0, has_side_effects=True),
            name="covariance",
        )(
            weights,
            fine.reshape(kf * lons, lats),
            coarse.reshape(kc * halves, lats),
            inc.reshape(nv * lons, lats),
        )
        return result.reshape(nv, lons, lats)

    spec = P(None, "lon", "lat")
    return jax.shard_map(
        per_device, mesh=mesh, in_specs=(spec, spec, spec, P()), out_specs=spec, check_vma=False
    )
```

```python
import functools

import jax
import jax.numpy as jnp
from jax import lax
from jax.experimental import pallas as pl
from jax.experimental.pallas import tpu as pltpu
from jax.sharding import PartitionSpec as P

MESH = pl.DeviceIdType.MESH
F32, BF16 = jnp.float32, jnp.bfloat16


def profile(distance, extent):
    ratio = distance.astype(F32) / extent
    return jnp.where(jnp.abs(distance) <= extent, 1.0 - 0.75 * ratio * ratio, 0.0)


def iota(shape, dim):
    return lax.broadcasted_iota(jnp.int32, shape, dim)


def kernel(
    sizes, weights_ref, fine_ref, coarse_ref, inc_ref, out_ref,
    w_ref, fine_in, coarse_in, inc_in, wide, wide_c, west_cin, east_cin, turned, rim_in,
    near_f, near_i, near_c, near_p, own_c, own_r, taper, rim_taper, own_rim, acc,
    in_sem, send_sem, recv_sem, rim_send_sem, rim_recv_sem, ok_sem,
):
    n_lon, n_lat, kf, kc, nv, lons, lats = sizes
    halves, reach, lon_reach = lons // 2, lats // 8, lons - 1
    ratio = (kc - 1) / (kf - 1)
    lon, lat = lax.axis_index("lon"), lax.axis_index("lat")
    sides = (lax.rem(lon + n_lon - 1, n_lon), lon, lax.rem(lon + 1, n_lon))
    has = (lat > 0, lat < n_lat - 1)
    odd = lax.rem(lat, 2) == 1
    even = jnp.logical_not(odd)
    one_side = n_lat == 2
    slots = range(1) if one_side else range(2)

    barrier = pltpu.get_barrier_semaphore()

    loads = [
        pltpu.make_async_copy(src, dst, in_sem.at[n])
        for n, (src, dst) in enumerate(
            ((coarse_ref, coarse_in), (fine_ref, fine_in), (inc_ref, inc_in), (weights_ref, w_ref))
        )
    ]
    for load in loads:
        load.start()

    def by_side(do):
        for s in range(2):
            if not one_side:
                pl.when(has[s])(functools.partial(do, s))
        if one_side:
            do(lax.rem(lat + 1, 2))

    def greet(to_lon, to_lat):
        pl.semaphore_signal(barrier, inc=1, device_id=(to_lon, to_lat), device_id_type=MESH)

    greet(sides[0], lat)
    greet(sides[2], lat)

    @pl.when(even)
    def _():
        by_side(lambda s: [greet(sides[t], lat + 2 * s - 1) for t in (1, 0, 2)] and None)

    def send(src, dst, sent, arrived, towards):
        return pltpu.make_async_remote_copy(
            src_ref=src, dst_ref=dst, send_sem=send_sem.at[sent], recv_sem=recv_sem.at[arrived],
            device_id=(sides[towards], lat), device_id_type=MESH,
        )

    first, past, last = lon_reach, lon_reach + lons, 2 * lon_reach + lons
    to_west, to_east = pl.ds(first, lon_reach), pl.ds(first + 1, lon_reach)
    from_west, from_east = pl.ds(0, lon_reach), pl.ds(past, lon_reach)
    coarse_west = send(coarse_in, east_cin, 0, 0, 0)
    coarse_east = send(coarse_in, west_cin, 0, 1, 2)
    fine_west = send(near_f.at[to_west], near_f.at[from_east], 1, 2, 0)
    fine_east = send(near_f.at[to_east], near_f.at[from_west], 1, 3, 2)
    inc_west = send(near_i.at[to_west], near_i.at[from_east], 1, 2, 0)
    inc_east = send(near_i.at[to_east], near_i.at[from_west], 1, 4, 2)

    def rim_copy(slot, t):
        towards = 1 - 2 * lat if one_side else 2 * slot - 1
        other = 0 if one_side else 1 - slot
        at = jnp.where(has[0], 0, lats - reach) if one_side else slot * (lats - reach)
        return pltpu.make_async_remote_copy(
            src_ref=turned.at[:, pl.ds(pl.multiple_of(at, reach), reach)], dst_ref=rim_in.at[other, 2 - t],
            send_sem=rim_send_sem.at[slot], recv_sem=rim_recv_sem.at[other],
            device_id=(lax.rem(lon + n_lon - 1 + t, n_lon), lat + towards), device_id_type=MESH,
        )

    def by_slot(do):
        for slot in slots:
            if one_side:
                do(slot)
            else:
                pl.when(has[slot])(functools.partial(do, slot))

    def rims_start(slot):
        ahead = lax.rem(lon, 2)
        for t in (1 + ahead, 2 - ahead, 0):
            rim_copy(slot, t).start()

    def drain(ref, sem):
        pltpu.make_async_copy(ref, ref, sem).wait()

    def rims_arrive(slot):
        drain(rim_in.at[slot], rim_recv_sem.at[slot])

    def rims_sent(slot):
        drain(rim_in.at[slot], rim_send_sem.at[slot])

    loads[0].wait()

    @pl.when(even)
    def _():
        pl.semaphore_wait(barrier, 2)
        coarse_east.start()
        coarse_west.start()

    def columns(source, slot):
        wide_c[slot] = source[...].astype(F32)
        return [wide_c[slot, pl.ds(c, kc, stride=halves), :] for c in range(halves)]

    f_at, i_at = 0, kf * lons
    loads[1].wait()
    loads[2].wait()
    coarse_own = columns(coarse_in, 0)
    wide[f_at:f_at + kf * lons] = fine_in[...].astype(F32)
    wide[i_at:i_at + nv * lons] = inc_in[...].astype(F32)
    centred = [v - jnp.mean(v, axis=0, keepdims=True) for v in coarse_own]
    fine_own, inc_own = [], []
    for a in range(lons):
        values = wide[pl.ds(f_at + a, kf, stride=lons), :]
        anom = (values - jnp.mean(values, axis=0, keepdims=True)).astype(BF16)
        vectors = wide[pl.ds(i_at + a, nv, stride=lons), :].astype(BF16)
        near_f[first + a] = anom
        near_i[first + a] = vectors
        fine_own.append(anom)
        inc_own.append(vectors)
    stacks = centred + [
        jnp.concatenate(own, axis=0) for own in (fine_own, inc_own)
    ]
    for n, stack in enumerate(stacks):
        turned[n] = stack.astype(BF16).T

    @pl.when(even)
    def _():
        fine_east.start()
        inc_east.start()
        fine_west.start()
        inc_west.start()

    if not one_side:
        for s in slots:
            @pl.when(jnp.logical_not(has[s]))
            def _():
                rim_in[s] = jnp.zeros(rim_in.shape[1:], BF16)

    one = jnp.int32(1)

    @pl.when(odd)
    def _():
        pl.semaphore_wait(barrier, 2 + 3 * jnp.where(has[0], one, 0) + 3 * jnp.where(has[1], one, 0))
        by_slot(rims_start)
        coarse_east.start()
        coarse_west.start()
        fine_east.start()
        inc_east.start()
        fine_west.start()
        inc_west.start()
        by_side(lambda s: pl.semaphore_signal(
            ok_sem.at[0 if one_side else 1 - s], inc=1, device_id=(lon, lat + 2 * s - 1), device_id_type=MESH
        ))

    loads[3].wait()
    w_coarse = w_ref[1] / (kc - 1)
    fine_ratio = ratio * w_ref[0] / w_ref[1]
    lat_profile = w_coarse * profile(iota((lats, lats), 0) - iota((lats, lats), 1), reach)
    for d in range(lon_reach + 1):
        taper[d] = lat_profile * (1.0 - 0.75 * (d / lon_reach) * (d / lon_reach))

    shape = (3 * reach, lats)
    row, lane = iota(shape, 0), iota(shape, 1)
    a_lane, i_lane = lane // (2 * reach), lane % reach
    side = 1 - (lane // reach) % 2
    d_lat = reach + (2 * side - 1) * (row % reach - i_lane)
    for slot in slots:
        mine = side == (jnp.where(has[0], 0, 1) if one_side else slot)
        in_lat = jnp.where(mine, w_coarse * profile(d_lat, reach), 0.0)
        for b in range(lons):
            d_lon = (row // reach - 1) * lons + b - a_lane
            rim_taper[slot, b] = in_lat * profile(d_lon, lon_reach)

    def coarse_parts(refined):
        coarse_anom = refined - jnp.mean(refined, axis=0, keepdims=True)
        pair = refined[:kf]
        paired = pair - jnp.mean(pair, axis=0, keepdims=True)
        return coarse_anom.astype(BF16), paired.astype(BF16)

    def set_near(b, refined):
        coarse_anom, paired = coarse_parts(refined)
        near_c[first + b] = coarse_anom
        near_p[first + b] = paired
        return coarse_anom, paired

    def split(scale, values):
        scaled = scale * values.astype(F32)
        high = scaled.astype(BF16).astype(F32)
        return [high, scaled - high]

    def set_own(a, refined):
        coarse_anom, paired = set_near(a, refined)
        if a % 2 == 0:
            own_c[a] = turned[a // 2]
        else:
            own_c[a] = coarse_anom.T
        rest = split(fine_ratio, near_f[first + a]) + split(-ratio, paired)
        own_r[a] = jnp.concatenate(rest, axis=0).astype(BF16).T

    def own_rows(lo, hi):
        return jnp.concatenate(
            [jnp.concatenate([own_c[a], own_r[a]], axis=1) for a in range(lo, hi)], axis=0
        )

    def members(coarse_anom, fine_anom, paired):
        return jnp.concatenate([coarse_anom, fine_anom, fine_anom, paired, paired], axis=0)

    def near(b):
        at = first + b
        return members(near_c[at], near_f[at], near_p[at])

    def product(rows, bs, lo, hi):
        gram = jnp.dot(
            own_rows(lo, hi), jnp.concatenate([near(b) for b in bs], axis=1),
            preferred_element_type=F32,
        )
        for n, b in enumerate(bs):
            for a in range(lo, hi):
                part = gram[(a - lo) * lats:(a - lo + 1) * lats, n * lats:(n + 1) * lats]
                rows[a, b] = (part * taper[abs(a - b)]).astype(BF16)

    def apply(rows, a):
        bs = sorted(b for row, b in rows if row == a)
        vectors = jnp.concatenate([near_i[first + b] for b in bs], axis=1)
        tapered = jnp.concatenate([rows[a, b] for b in bs], axis=1)
        return lax.dot_general(
            vectors, tapered, (((1,), (1,)), ((), ())), preferred_element_type=F32
        )

    def middle(cols, b):
        return cols[b // 2] if b % 2 == 0 else 0.5 * (cols[b // 2] + cols[b // 2 + 1])

    for a in range(lon_reach):
        set_own(a, middle(coarse_own, a))
    rows = {}
    product(rows, tuple(range(lon_reach)), 0, lon_reach)
    for a in range(lon_reach):
        acc[a] = apply(rows, a)

    @pl.when(even)
    def _():
        by_side(lambda s: pl.semaphore_wait(ok_sem.at[0 if one_side else s], 1))
        by_slot(rims_start)

    coarse_west.wait_recv()
    east_c = columns(east_cin, 1)
    set_own(lon_reach, 0.5 * (coarse_own[halves - 1] + east_c[0]))
    rows = {}
    product(rows, tuple(range(lon_reach)), lon_reach, lons)
    product(rows, (lon_reach,), 0, lons)
    for b in range(lon_reach):
        set_near(lons + b, middle(east_c, b))
    for a in range(lon_reach):
        acc[a] += apply(rows, a)
    acc[lon_reach] = apply(rows, lon_reach)
    drain(near_f.at[pl.ds(0, 2 * lon_reach)], recv_sem.at[2])
    rows = {}
    for b in range(0, lon_reach, 2):
        pair = tuple(lons + n for n in range(b, min(b + 2, lon_reach)))
        if len(pair) == 2:
            product(rows, pair[:1], b + 1, b + 2)
        product(rows, pair, b + len(pair), lons)
    for a in range(1, lons):
        acc[a] += apply(rows, a)

    c_rows, r_rows = (
        jnp.concatenate(
            [own[a, at:at + reach] for a in range(lons) for at in (lats - reach, 0)], axis=0
        ).astype(F32)
        for own in (own_c, own_r)
    )
    lead = iota((lats, kc), 1) < kf
    paired = pltpu.roll(r_rows, lats - 2 * kf, 1) + pltpu.roll(r_rows, lats - 3 * kf, 1)
    c_rows += jnp.where(lead, paired, 0.0)
    fine_rows = jnp.where(lead, r_rows, 0.0)
    fine_rows += pltpu.roll(fine_rows, kf, 1)
    fine_rows += pltpu.roll(fine_rows, 2 * kf, 1)
    own_rim[:, :kc] = c_rows.astype(BF16)
    own_rim[:, kc:] = fine_rows.astype(BF16)

    coarse_east.wait_recv()
    west_c = columns(west_cin, 2)
    west_c.append(coarse_own[0])
    for b in range(1, lons):
        set_near(b - lons, middle(west_c, b))

    def average(x, y):
        return (0.5 * (x.astype(F32) + y.astype(F32))).astype(BF16)

    def rim_taps(slot):
        group = iota((reach, lats), 1) // kf
        taps = []
        for pair in range(0, lons, 2):
            cells = []
            for b in (pair, pair + 1):
                for t in range(3):
                    cols = [rim_in[slot, t, c] for c in range(halves)]
                    cols.append(rim_in[slot, min(t + 1, 2), 0])
                    coarse = cols[b // 2] if b % 2 == 0 else average(cols[b // 2], cols[b // 2 + 1])
                    fine = jnp.where(group == b, rim_in[slot, t, halves].astype(F32), 0.0)
                    cells.append(jnp.concatenate([coarse, fine.astype(BF16)], axis=1))
            gram = lax.dot_general(
                jnp.concatenate(cells, axis=0), own_rim[...], (((1,), (1,)), ((), ())),
                preferred_element_type=F32,
            )
            for e in range(2):
                part = gram[3 * reach * e:3 * reach * (e + 1)]
                taps.append((part * rim_taper[slot, pair + e]).astype(BF16))
                taps.append(jnp.zeros((reach, lats), BF16))
        return jnp.concatenate(taps, axis=0)

    def rim_vectors(slot):
        cells = [rim_in[slot, t, halves + 1] for t in range(3)]
        cells = (cells + [jnp.zeros((reach, lats), BF16)]) * 2
        cells = jnp.concatenate(cells, axis=0).T.astype(F32)
        lower = iota((nv, lats), 1) < lats // 2
        pairs = [
            jnp.where(lower, cells[b * nv:(b + 1) * nv], cells[(b + 1) * nv:(b + 2) * nv])
            for b in range(0, lons, 2)
        ]
        return jnp.concatenate(pairs, axis=1).astype(BF16)

    drain(wide_c.at[0], send_sem.at[0])
    drain(turned.at[pl.ds(0, 3)], send_sem.at[1])
    fine_east.wait_recv()
    rows = {}
    for b in range(lons - 1, 0, -2):
        pair = tuple(n - lons for n in range(b, max(b - 2, 0), -1))
        product(rows, pair, 0, b + 1 - len(pair))
        if len(pair) == 2:
            product(rows, pair[:1], b - 1, b)
    by_slot(rims_arrive)
    vectors = [rim_vectors(slot) for slot in slots]
    taps = [rim_taps(slot) for slot in slots]
    inc_east.wait_recv()
    edge = functools.reduce(
        jnp.add,
        [
            jnp.dot(
                vectors[slot][:, at:at + lats], taps[slot][at:at + lats],
                preferred_element_type=F32,
            )
            for slot in slots
            for at in (0, lats)
        ],
    )
    total = [acc[a] + apply(rows, a) for a in range(lon_reach)] + [acc[lon_reach]]
    lane = iota((nv, lats), 1)
    at_edge = (lane < reach) | (lane >= lats - reach)
    for a in range(lons):
        rim = pltpu.roll(edge, (lats - reach - 2 * reach * a) % lats, 1)
        out_ref[pl.ds(a, nv, stride=lons), :] = total[a] + jnp.where(at_edge, rim, 0.0)

    by_slot(rims_sent)


def solution(mesh):
    n_lon, n_lat = mesh.shape["lon"], mesh.shape["lat"]

    def per_device(fine, coarse, inc, weights):
        kf, lons, lats = fine.shape
        kc, halves, _ = coarse.shape
        nv = inc.shape[0]
        near_lons = 3 * lons - 2
        slots = 1 if n_lat == 2 else 2
        assert lons == 4 and nv == kf and lats == kc == 4 * kf
        result = pl.pallas_call(
            functools.partial(kernel, (n_lon, n_lat, kf, kc, nv, lons, lats)),
            out_shape=pltpu.VMEM((nv * lons, lats), F32),
            in_specs=[pl.BlockSpec(memory_space=pl.ANY)] * 4,
            out_specs=pl.BlockSpec(memory_space=pltpu.VMEM),
            scratch_shapes=[
                pltpu.SMEM(weights.shape, F32),
                pltpu.VMEM((kf * lons, lats), BF16),
                pltpu.VMEM((kc * halves, lats), BF16),
                pltpu.VMEM((nv * lons, lats), BF16),
                pltpu.VMEM(((kf + nv) * lons, lats), F32),
                pltpu.VMEM((3, kc * halves, lats), F32),
                pltpu.VMEM((kc * halves, lats), BF16),
                pltpu.VMEM((kc * halves, lats), BF16),
                pltpu.VMEM((halves + 2, lats, kc), BF16),
                pltpu.VMEM((slots, 3, halves + 2, lats // 8, kc), BF16),
                pltpu.VMEM((near_lons, kf, lats), BF16),
                pltpu.VMEM((near_lons, nv, lats), BF16),
                pltpu.VMEM((near_lons, kc, lats), BF16),
                pltpu.VMEM((near_lons, kf, lats), BF16),
                pltpu.VMEM((lons, lats, kc), BF16),
                pltpu.VMEM((lons, lats, 4 * kf), BF16),
                pltpu.VMEM((lons, lats, lats), F32),
                pltpu.VMEM((slots, lons, 3 * lats // 8, lats), F32),
                pltpu.VMEM((lats, 2 * lats), BF16),
                pltpu.VMEM((lons, nv, lats), F32),
                pltpu.SemaphoreType.DMA((4,)),
                pltpu.SemaphoreType.DMA((2,)),
                pltpu.SemaphoreType.DMA((5,)),
                pltpu.SemaphoreType.DMA((slots,)),
                pltpu.SemaphoreType.DMA((slots,)),
                pltpu.SemaphoreType.REGULAR((slots,)),
            ],
            compiler_params=pltpu.CompilerParams(collective_id=0, has_side_effects=True),
            name="covariance",
        )(
            weights,
            fine.reshape(kf * lons, lats),
            coarse.reshape(kc * halves, lats),
            inc.reshape(nv * lons, lats),
        )
        return result.reshape(nv, lons, lats)

    spec = P(None, "lon", "lat")
    return jax.shard_map(
        per_device, mesh=mesh, in_specs=(spec, spec, spec, P()), out_specs=spec, check_vma=False
    )
```

```python
import functools

import jax
import jax.numpy as jnp
from jax import lax
from jax.experimental import pallas as pl
from jax.experimental.pallas import tpu as pltpu
from jax.sharding import PartitionSpec as P

MESH = pl.DeviceIdType.MESH
F32, BF16 = jnp.float32, jnp.bfloat16


def profile(distance, extent):
    ratio = distance.astype(F32) / extent
    return jnp.where(jnp.abs(distance) <= extent, 1.0 - 0.75 * ratio * ratio, 0.0)


def iota(shape, dim):
    return lax.broadcasted_iota(jnp.int32, shape, dim)


def kernel(
    sizes, weights_ref, fine_ref, coarse_ref, inc_ref, out_ref,
    w_ref, fine_in, coarse_in, inc_in, wide, wide_c, west_cin, east_cin, turned, rim_in,
    near_f, near_i, near_c, near_p, own_c, own_r, taper, rim_taper, own_rim, acc,
    in_sem, send_sem, recv_sem, rim_send_sem, rim_recv_sem, ok_sem,
):
    n_lon, n_lat, kf, kc, nv, lons, lats = sizes
    halves, reach, lon_reach = lons // 2, lats // 8, lons - 1
    ratio = (kc - 1) / (kf - 1)
    lon, lat = lax.axis_index("lon"), lax.axis_index("lat")
    sides = (lax.rem(lon + n_lon - 1, n_lon), lon, lax.rem(lon + 1, n_lon))
    has = (lat > 0, lat < n_lat - 1)
    odd = lax.rem(lat, 2) == 1
    even = jnp.logical_not(odd)
    one_side = n_lat == 2
    slots = range(1) if one_side else range(2)

    barrier = pltpu.get_barrier_semaphore()

    loads = [
        pltpu.make_async_copy(src, dst, in_sem.at[n])
        for n, src, dst in (
            (0, coarse_ref, coarse_in), (1, fine_ref, fine_in), (1, inc_ref, inc_in),
            (2, weights_ref, w_ref),
        )
    ]
    for load in loads:
        load.start()

    def by_side(do):
        for s in range(2):
            if not one_side:
                pl.when(has[s])(functools.partial(do, s))
        if one_side:
            do(lax.rem(lat + 1, 2))

    def greet(to_lon, to_lat):
        pl.semaphore_signal(barrier, inc=1, device_id=(to_lon, to_lat), device_id_type=MESH)

    greet(sides[0], lat)
    greet(sides[2], lat)

    @pl.when(even)
    def _():
        by_side(lambda s: [greet(sides[t], lat + 2 * s - 1) for t in (1, 0, 2)] and None)

    def send(src, dst, sent, arrived, towards):
        return pltpu.make_async_remote_copy(
            src_ref=src, dst_ref=dst, send_sem=send_sem.at[sent], recv_sem=recv_sem.at[arrived],
            device_id=(sides[towards], lat), device_id_type=MESH,
        )

    first, past, last = lon_reach, lon_reach + lons, 2 * lon_reach + lons
    to_west, to_east = pl.ds(first, lon_reach), pl.ds(first + 1, lon_reach)
    from_west, from_east = pl.ds(0, lon_reach), pl.ds(past, lon_reach)
    coarse_west = send(coarse_in, east_cin, 0, 0, 0)
    coarse_east = send(coarse_in, west_cin, 0, 1, 2)
    fine_west = send(near_f.at[to_west], near_f.at[from_east], 1, 2, 0)
    fine_east = send(near_f.at[to_east], near_f.at[from_west], 1, 3, 2)
    inc_west = send(near_i.at[to_west], near_i.at[from_east], 1, 2, 0)
    inc_east = send(near_i.at[to_east], near_i.at[from_west], 1, 4, 2)

    def rim_copy(slot, t):
        towards = 1 - 2 * lat if one_side else 2 * slot - 1
        other = 0 if one_side else 1 - slot
        at = jnp.where(has[0], 0, lats - reach) if one_side else slot * (lats - reach)
        return pltpu.make_async_remote_copy(
            src_ref=turned.at[:, pl.ds(pl.multiple_of(at, reach), reach)], dst_ref=rim_in.at[other, 2 - t],
            send_sem=rim_send_sem.at[slot], recv_sem=rim_recv_sem.at[other],
            device_id=(lax.rem(lon + n_lon - 1 + t, n_lon), lat + towards), device_id_type=MESH,
        )

    def by_slot(do):
        for slot in slots:
            if one_side:
                do(slot)
            else:
                pl.when(has[slot])(functools.partial(do, slot))

    def rims_start(slot):
        ahead = lax.rem(lon, 2)
        for t in (1 + ahead, 2 - ahead, 0):
            rim_copy(slot, t).start()

    def drain(ref, sem):
        pltpu.make_async_copy(ref, ref, sem).wait()

    def rims_arrive(slot):
        drain(rim_in.at[slot], rim_recv_sem.at[slot])

    def rims_sent(slot):
        drain(rim_in.at[slot], rim_send_sem.at[slot])

    loads[0].wait()

    @pl.when(even)
    def _():
        pl.semaphore_wait(barrier, 2)
        coarse_east.start()
        coarse_west.start()

    def columns(source, slot):
        wide_c[slot] = source[...].astype(F32)
        return [wide_c[slot, pl.ds(c, kc, stride=halves), :] for c in range(halves)]

    f_at, i_at = 0, kf * lons
    drain(turned.at[pl.ds(0, 2)], in_sem.at[1])
    coarse_own = columns(coarse_in, 0)
    wide[f_at:f_at + kf * lons] = fine_in[...].astype(F32)
    wide[i_at:i_at + nv * lons] = inc_in[...].astype(F32)
    centred = [v - jnp.mean(v, axis=0, keepdims=True) for v in coarse_own]
    fine_own, inc_own = [], []
    for a in range(lons):
        values = wide[pl.ds(f_at + a, kf, stride=lons), :]
        anom = (values - jnp.mean(values, axis=0, keepdims=True)).astype(BF16)
        vectors = wide[pl.ds(i_at + a, nv, stride=lons), :].astype(BF16)
        near_f[first + a] = anom
        near_i[first + a] = vectors
        fine_own.append(anom)
        inc_own.append(vectors)
    stacks = centred + [
        jnp.concatenate(own, axis=0) for own in (fine_own, inc_own)
    ]
    for n, stack in enumerate(stacks):
        turned[n] = stack.astype(BF16).T

    @pl.when(even)
    def _():
        fine_east.start()
        inc_east.start()
        fine_west.start()
        inc_west.start()

    if not one_side:
        for s in slots:
            @pl.when(jnp.logical_not(has[s]))
            def _():
                rim_in[s] = jnp.zeros(rim_in.shape[1:], BF16)

    one = jnp.int32(1)

    @pl.when(odd)
    def _():
        pl.semaphore_wait(barrier, 2 + 3 * jnp.where(has[0], one, 0) + 3 * jnp.where(has[1], one, 0))
        by_slot(rims_start)
        coarse_east.start()
        coarse_west.start()
        fine_east.start()
        inc_east.start()
        fine_west.start()
        inc_west.start()
        by_side(lambda s: pl.semaphore_signal(
            ok_sem.at[0 if one_side else 1 - s], inc=1, device_id=(lon, lat + 2 * s - 1), device_id_type=MESH
        ))

    loads[3].wait()
    w_coarse = w_ref[1] / (kc - 1)
    fine_ratio = ratio * w_ref[0] / w_ref[1]
    lat_profile = w_coarse * profile(iota((lats, lats), 0) - iota((lats, lats), 1), reach)
    for d in range(lon_reach + 1):
        taper[d] = lat_profile * (1.0 - 0.75 * (d / lon_reach) * (d / lon_reach))

    shape = (3 * reach, lats)
    row, lane = iota(shape, 0), iota(shape, 1)
    a_lane, i_lane = lane // (2 * reach), lane % reach
    side = 1 - (lane // reach) % 2
    d_lat = reach + (2 * side - 1) * (row % reach - i_lane)
    for slot in slots:
        mine = side == (jnp.where(has[0], 0, 1) if one_side else slot)
        in_lat = jnp.where(mine, w_coarse * profile(d_lat, reach), 0.0)
        for b in range(lons):
            d_lon = (row // reach - 1) * lons + b - a_lane
            rim_taper[slot, b] = in_lat * profile(d_lon, lon_reach)

    def coarse_parts(refined):
        coarse_anom = refined - jnp.mean(refined, axis=0, keepdims=True)
        pair = refined[:kf]
        paired = pair - jnp.mean(pair, axis=0, keepdims=True)
        return coarse_anom.astype(BF16), paired.astype(BF16)

    def set_near(b, refined):
        coarse_anom, paired = coarse_parts(refined)
        near_c[first + b] = coarse_anom
        near_p[first + b] = paired
        return coarse_anom, paired

    def split(scale, values):
        scaled = scale * values.astype(F32)
        high = scaled.astype(BF16).astype(F32)
        return [high, scaled - high]

    def set_own(a, refined):
        coarse_anom, paired = set_near(a, refined)
        if a % 2 == 0:
            own_c[a] = turned[a // 2]
        else:
            own_c[a] = coarse_anom.T
        rest = split(fine_ratio, near_f[first + a]) + split(-ratio, paired)
        own_r[a] = jnp.concatenate(rest, axis=0).astype(BF16).T

    def own_rows(lo, hi):
        return jnp.concatenate(
            [jnp.concatenate([own_c[a], own_r[a]], axis=1) for a in range(lo, hi)], axis=0
        )

    def members(coarse_anom, fine_anom, paired):
        return jnp.concatenate([coarse_anom, fine_anom, fine_anom, paired, paired], axis=0)

    def near(b):
        at = first + b
        return members(near_c[at], near_f[at], near_p[at])

    def product(rows, bs, lo, hi):
        gram = jnp.dot(
            own_rows(lo, hi), jnp.concatenate([near(b) for b in bs], axis=1),
            preferred_element_type=F32,
        )
        for n, b in enumerate(bs):
            for a in range(lo, hi):
                part = gram[(a - lo) * lats:(a - lo + 1) * lats, n * lats:(n + 1) * lats]
                rows[a, b] = (part * taper[abs(a - b)]).astype(BF16)

    def apply(rows, a):
        bs = sorted(b for row, b in rows if row == a)
        vectors = jnp.concatenate([near_i[first + b] for b in bs], axis=1)
        tapered = jnp.concatenate([rows[a, b] for b in bs], axis=1)
        return lax.dot_general(
            vectors, tapered, (((1,), (1,)), ((), ())), preferred_element_type=F32
        )

    def middle(cols, b):
        return cols[b // 2] if b % 2 == 0 else 0.5 * (cols[b // 2] + cols[b // 2 + 1])

    for a in range(lon_reach):
        set_own(a, middle(coarse_own, a))
    rows = {}
    product(rows, tuple(range(lon_reach)), 0, lon_reach)
    for a in range(lon_reach):
        acc[a] = apply(rows, a)

    @pl.when(even)
    def _():
        by_side(lambda s: pl.semaphore_wait(ok_sem.at[0 if one_side else s], 1))
        by_slot(rims_start)

    coarse_west.wait_recv()
    east_c = columns(east_cin, 1)
    set_own(lon_reach, 0.5 * (coarse_own[halves - 1] + east_c[0]))
    rows = {}
    product(rows, tuple(range(lon_reach)), lon_reach, lons)
    product(rows, (lon_reach,), 0, lons)
    for b in range(lon_reach):
        set_near(lons + b, middle(east_c, b))
    for a in range(lon_reach):
        acc[a] += apply(rows, a)
    acc[lon_reach] = apply(rows, lon_reach)
    drain(near_f.at[pl.ds(0, 2 * lon_reach)], recv_sem.at[2])
    rows = {}
    for b in range(0, lon_reach, 2):
        pair = tuple(lons + n for n in range(b, min(b + 2, lon_reach)))
        if len(pair) == 2:
            product(rows, pair[:1], b + 1, b + 2)
        product(rows, pair, b + len(pair), lons)
    for a in range(1, lons):
        acc[a] += apply(rows, a)

    c_rows, r_rows = (
        jnp.concatenate(
            [own[a, at:at + reach] for a in range(lons) for at in (lats - reach, 0)], axis=0
        ).astype(F32)
        for own in (own_c, own_r)
    )
    lead = iota((lats, kc), 1) < kf
    paired = pltpu.roll(r_rows, lats - 2 * kf, 1) + pltpu.roll(r_rows, lats - 3 * kf, 1)
    c_rows += jnp.where(lead, paired, 0.0)
    fine_rows = jnp.where(lead, r_rows, 0.0)
    fine_rows += pltpu.roll(fine_rows, kf, 1)
    fine_rows += pltpu.roll(fine_rows, 2 * kf, 1)
    own_rim[:, :kc] = c_rows.astype(BF16)
    own_rim[:, kc:] = fine_rows.astype(BF16)

    coarse_east.wait_recv()
    west_c = columns(west_cin, 2)
    west_c.append(coarse_own[0])
    for b in range(1, lons):
        set_near(b - lons, middle(west_c, b))

    def average(x, y):
        return (0.5 * (x.astype(F32) + y.astype(F32))).astype(BF16)

    def rim_taps(slot):
        group = iota((reach, lats), 1) // kf
        taps = []
        for pair in range(0, lons, 2):
            cells, places = [], []
            for b in (pair, pair + 1):
                for t in range(3):
                    if (t, b) in ((0, 0), (2, lons - 1)):
                        continue
                    places.append((b, t))
                    cols = [rim_in[slot, t, c] for c in range(halves)]
                    cols.append(rim_in[slot, min(t + 1, 2), 0])
                    coarse = cols[b // 2] if b % 2 == 0 else average(cols[b // 2], cols[b // 2 + 1])
                    fine = jnp.where(group == b, rim_in[slot, t, halves].astype(F32), 0.0)
                    cells.append(jnp.concatenate([coarse, fine.astype(BF16)], axis=1))
            gram = lax.dot_general(
                jnp.concatenate(cells, axis=0), own_rim[...], (((1,), (1,)), ((), ())),
                preferred_element_type=F32,
            )
            for b in (pair, pair + 1):
                for t in range(4):
                    if (b, t) not in places:
                        taps.append(jnp.zeros((reach, lats), BF16))
                        continue
                    at = reach * places.index((b, t))
                    weight = rim_taper[slot, b, t * reach:(t + 1) * reach]
                    taps.append((gram[at:at + reach] * weight).astype(BF16))
        return jnp.concatenate(taps, axis=0)

    def rim_vectors(slot):
        cells = [rim_in[slot, t, halves + 1] for t in range(3)]
        cells = (cells + [jnp.zeros((reach, lats), BF16)]) * 2
        cells = jnp.concatenate(cells, axis=0).T.astype(F32)
        lower = iota((nv, lats), 1) < lats // 2
        pairs = [
            jnp.where(lower, cells[b * nv:(b + 1) * nv], cells[(b + 1) * nv:(b + 2) * nv])
            for b in range(0, lons, 2)
        ]
        return jnp.concatenate(pairs, axis=1).astype(BF16)

    drain(wide_c.at[0], send_sem.at[0])
    drain(turned.at[pl.ds(0, 3)], send_sem.at[1])
    fine_east.wait_recv()
    rows = {}
    for b in range(lons - 1, 0, -2):
        pair = tuple(n - lons for n in range(b, max(b - 2, 0), -1))
        product(rows, pair, 0, b + 1 - len(pair))
        if len(pair) == 2:
            product(rows, pair[:1], b - 1, b)
    by_slot(rims_arrive)
    vectors = [rim_vectors(slot) for slot in slots]
    taps = [rim_taps(slot) for slot in slots]
    inc_east.wait_recv()
    edge = functools.reduce(
        jnp.add,
        [
            jnp.dot(
                vectors[slot][:, at:at + lats], taps[slot][at:at + lats],
                preferred_element_type=F32,
            )
            for slot in slots
            for at in (0, lats)
        ],
    )
    total = [acc[a] + apply(rows, a) for a in range(lon_reach)] + [acc[lon_reach]]
    lane = iota((nv, lats), 1)
    at_edge = (lane < reach) | (lane >= lats - reach)
    for a in range(lons):
        rim = pltpu.roll(edge, (lats - reach - 2 * reach * a) % lats, 1)
        out_ref[pl.ds(a, nv, stride=lons), :] = total[a] + jnp.where(at_edge, rim, 0.0)

    by_slot(rims_sent)


def solution(mesh):
    n_lon, n_lat = mesh.shape["lon"], mesh.shape["lat"]

    def per_device(fine, coarse, inc, weights):
        kf, lons, lats = fine.shape
        kc, halves, _ = coarse.shape
        nv = inc.shape[0]
        near_lons = 3 * lons - 2
        slots = 1 if n_lat == 2 else 2
        assert lons == 4 and nv == kf and lats == kc == 4 * kf
        result = pl.pallas_call(
            functools.partial(kernel, (n_lon, n_lat, kf, kc, nv, lons, lats)),
            out_shape=pltpu.VMEM((nv * lons, lats), F32),
            in_specs=[pl.BlockSpec(memory_space=pl.ANY)] * 4,
            out_specs=pl.BlockSpec(memory_space=pltpu.VMEM),
            scratch_shapes=[
                pltpu.SMEM(weights.shape, F32),
                pltpu.VMEM((kf * lons, lats), BF16),
                pltpu.VMEM((kc * halves, lats), BF16),
                pltpu.VMEM((nv * lons, lats), BF16),
                pltpu.VMEM(((kf + nv) * lons, lats), F32),
                pltpu.VMEM((3, kc * halves, lats), F32),
                pltpu.VMEM((kc * halves, lats), BF16),
                pltpu.VMEM((kc * halves, lats), BF16),
                pltpu.VMEM((halves + 2, lats, kc), BF16),
                pltpu.VMEM((slots, 3, halves + 2, lats // 8, kc), BF16),
                pltpu.VMEM((near_lons, kf, lats), BF16),
                pltpu.VMEM((near_lons, nv, lats), BF16),
                pltpu.VMEM((near_lons, kc, lats), BF16),
                pltpu.VMEM((near_lons, kf, lats), BF16),
                pltpu.VMEM((lons, lats, kc), BF16),
                pltpu.VMEM((lons, lats, 4 * kf), BF16),
                pltpu.VMEM((lons, lats, lats), F32),
                pltpu.VMEM((slots, lons, 3 * lats // 8, lats), F32),
                pltpu.VMEM((lats, 2 * lats), BF16),
                pltpu.VMEM((lons, nv, lats), F32),
                pltpu.SemaphoreType.DMA((3,)),
                pltpu.SemaphoreType.DMA((2,)),
                pltpu.SemaphoreType.DMA((5,)),
                pltpu.SemaphoreType.DMA((slots,)),
                pltpu.SemaphoreType.DMA((slots,)),
                pltpu.SemaphoreType.REGULAR((slots,)),
            ],
            compiler_params=pltpu.CompilerParams(collective_id=0, has_side_effects=True),
            name="covariance",
        )(
            weights,
            fine.reshape(kf * lons, lats),
            coarse.reshape(kc * halves, lats),
            inc.reshape(nv * lons, lats),
        )
        return result.reshape(nv, lons, lats)

    spec = P(None, "lon", "lat")
    return jax.shard_map(
        per_device, mesh=mesh, in_specs=(spec, spec, spec, P()), out_specs=spec, check_vma=False
    )
```
